32 devices in a mesh: groups: 2 (over y), seq: 8 (over z, core), panel: 2 (over x).
Axes of the slice: x: 2, y: 2, z: 4, core: 2. Of those that a mesh axis runs over, the one named last changes fastest.
Arguments:
- queries: bfloat16 [4096, 3072], P(('groups', 'seq'), 'panel'), parts along dimension 0, may hold values from -120 to 120
- key_rows: bfloat16 [4096, 3072], P(('groups', 'seq'), 'panel'), parts along dimension 0, may hold values from -6 to 6
- value_rows: bfloat16 [4096, 3072], P(('groups', 'seq'), 'panel'), parts along dimension 0, may hold values from -6 to 6
- block_lists: int32 [24, 16, 8], P('panel'), may hold values from 0 to 15, as said below
- block_counts: int32 [24, 16], P('panel'), may hold values from 4 to 8, as said below
Outputs:
- attended: bfloat16 [4096, 3072], P(('groups', 'seq', 'panel')), parts along dimension 0
The draws below stay inside these ranges and needn't reach their ends.
There are 2 independent parts, one for each index of `groups`. The reference program is written for one: setup_inputs(seed, part) draws one part's arguments, and reference() takes and returns one part's arrays. A program takes and returns all parts, laid end to end along the dimension named above; an argument that names none is the same for every part. Nothing has to cross between parts.
Inputs may be any that keep to these rules, and one draw needn't show every extreme that they name: `block_lists`: entry 0 of each list is the tile's own block index; the entries of one list are distinct; for each head, the lists of the 2 tiles held by one index of seq name together at most 1 distinct blocks among the 2 blocks of any other index of seq, and exactly 1 of some other index. `block_counts`: some list has all 8 entries live.
All inputs are finite; a program needn't handle non-finite values.
Results may differ from the reference program's by a relative error of at most 0.008.
Values may be sent and summed in bfloat16 or wider, within the bound.
No kernel may reach another device: no remote copies, remote signals or barrier semaphores. Data moves between devices by JAX's collectives and lax.ppermute only.
A program may use at most 128 MiB of HBM per device.

```python
import jax
import jax.numpy as jnp
from jax import lax

HEADS = 24
HEAD_DIM = 128
BLOCK = 128
TOK_DEV = 256
TOKENS = 2048
TILES = 16
LISTED = 8
SLOTS = 1


def query_key_pair(key):
    base = jax.random.fold_in(key, 7)
    key_part = jax.random.normal(jax.random.fold_in(base, 1), (TOKENS, HEADS * HEAD_DIM), jnp.float32)
    key_part = jnp.clip(key_part, -5.0, 5.0)
    query_part = jnp.clip(jax.random.normal(jax.random.fold_in(base, 2), (TOKENS, HEADS * HEAD_DIM), jnp.float32), -5.0, 5.0)
    return (query_part, key_part)


def draw_queries(key, part):
    return query_key_pair(key)[0].astype(jnp.bfloat16)


def draw_key_rows(key, part):
    return query_key_pair(key)[1].astype(jnp.bfloat16)


def draw_block_lists(key, part):
    base = jax.random.fold_in(key, 11)
    owned = TOK_DEV // BLOCK
    peers = TILES // owned
    width = owned + SLOTS * (peers - 1)
    pick_bits = jax.random.randint(jax.random.fold_in(base, 1), (HEADS, peers, peers, owned), 0, 1 << 20)
    pick_scores = pick_bits * owned + jnp.arange(owned, dtype=jnp.int32)[None, None, None, :]
    picked = jnp.argsort(pick_scores, axis=-1)[..., :SLOTS].astype(jnp.int32)
    chosen = picked + (jnp.arange(peers, dtype=jnp.int32) * owned)[None, None, :, None]
    peer_rows = jnp.arange(peers, dtype=jnp.int32)
    other_index = jnp.arange(peers - 1, dtype=jnp.int32)[None, :] + (jnp.arange(peers - 1, dtype=jnp.int32)[None, :] >= peer_rows[:, None]).astype(jnp.int32)
    others = jnp.take_along_axis(chosen, jnp.broadcast_to(other_index[None, :, :, None], (HEADS, peers, peers - 1, SLOTS)), axis=2)
    others = others.reshape(HEADS, peers, (peers - 1) * SLOTS)
    own_ids = peer_rows[:, None] * owned + jnp.arange(owned, dtype=jnp.int32)[None, :]
    candidates = jnp.concatenate([jnp.broadcast_to(own_ids[None], (HEADS, peers, owned)), others], axis=-1)
    per_tile = jnp.repeat(candidates, owned, axis=1)
    tile_ids = jnp.arange(TILES, dtype=jnp.int32)
    place = tile_ids % owned
    device = tile_ids // owned
    spots = jnp.arange(width - 1, dtype=jnp.int32)
    keep_index = spots[None, :] + (spots[None, :] >= place[:, None]).astype(jnp.int32)
    rest = jnp.take_along_axis(per_tile, jnp.broadcast_to(keep_index[None], (HEADS, TILES, width - 1)), axis=2)
    bits = jax.random.randint(jax.random.fold_in(base, 2), (HEADS, TILES, width - 1), 0, 1 << 20)
    scores = (bits + 1) * width + spots[None, None, :]
    favored_peer = jnp.where(device == peers - 1, 0, device)
    first_spot = owned - 1 + favored_peer * SLOTS
    favored = (spots[None, :] >= first_spot[:, None]) & (spots[None, :] < first_spot[:, None] + SLOTS) & (place[:, None] == 0)
    scores = jnp.where(favored[None], jnp.broadcast_to(spots[None, None, :], scores.shape), scores)
    order = jnp.argsort(scores, axis=-1)[:, :, :LISTED - 1].astype(jnp.int32)
    rest_taken = jnp.take_along_axis(rest, order, axis=2)
    own = jnp.broadcast_to(tile_ids[None, :, None], (HEADS, TILES, 1))
    return jnp.concatenate([own, rest_taken], axis=-1).astype(jnp.int32)


def draw_block_counts(key, part):
    base = jax.random.fold_in(key, 13)
    counts = jax.random.randint(base, (HEADS, TILES), LISTED // 2, LISTED + 1)
    head_pick = jax.random.randint(jax.random.fold_in(base, 1), (), 0, HEADS)
    tile_pick = jax.random.randint(jax.random.fold_in(base, 2), (), 0, TILES)
    return counts.at[head_pick, tile_pick].set(LISTED).astype(jnp.int32)


def levels(stream_key, extent, cuts, low, top_value):
    factor_of, own = 1.0, jax.random.fold_in(stream_key, 6)
    for axis_at, parts in cuts:
        draws = jnp.exp(jax.random.uniform(jax.random.fold_in(own, axis_at), (parts,), jnp.float32, low / len(cuts), top_value / len(cuts)))
        factor_of = factor_of * jnp.repeat(draws, extent[axis_at] // parts).reshape([-1 if axis == axis_at else 1 for axis in range(len(extent))])
    return factor_of


def bell_draw(stream_key, shape, deviation, bound, shards=(), kind=jnp.bfloat16):
    values = jax.random.normal(stream_key, shape, jnp.float32) * deviation
    if len(shards) > 0:
        values = levels(stream_key, shape, shards, -0.22, 0.18) * values
    return jnp.clip(values, min=-bound, max=bound).astype(kind)


def setup_inputs(seed: int = 0, part: int = 0) -> dict:
    key_list = jax.random.split(jax.random.key(seed), 6)
    own_keys = jax.random.split(jax.random.fold_in(key_list[5], part), 6)
    queries = draw_queries(jax.random.fold_in(jax.random.fold_in(key_list[5], part), 71), part)
    key_rows = draw_key_rows(jax.random.fold_in(jax.random.fold_in(key_list[5], part), 71), part)
    value_rows = bell_draw(own_keys[2], (TOKENS, HEADS * HEAD_DIM), 1.0, 6.0, ((0, 8), (1, 2)))
    block_lists = draw_block_lists(jax.random.fold_in(key_list[5], 71), part)
    block_counts = draw_block_counts(jax.random.fold_in(key_list[5], 71), part)
    return dict(queries=queries, key_rows=key_rows, value_rows=value_rows, block_lists=block_lists, block_counts=block_counts)


def reference(queries, key_rows, value_rows, block_lists, block_counts):
    tiles = queries.shape[0] // BLOCK
    scale = HEAD_DIM ** -0.5
    query_four = queries.reshape(tiles, BLOCK, HEADS, HEAD_DIM)
    key_four = key_rows.reshape(tiles, BLOCK, HEADS, HEAD_DIM)
    value_four = value_rows.reshape(tiles, BLOCK, HEADS, HEAD_DIM)
    live = jnp.arange(LISTED, dtype=jnp.int32)[None, None, :] < block_counts[:, :, None]

    def one_head(head):
        query_head = lax.dynamic_index_in_dim(query_four, head, 2, keepdims=False)
        key_head = lax.dynamic_index_in_dim(key_four, head, 2, keepdims=False)
        value_head = lax.dynamic_index_in_dim(value_four, head, 2, keepdims=False)
        listed = lax.dynamic_index_in_dim(block_lists, head, 0, keepdims=False)
        live_head = lax.dynamic_index_in_dim(live, head, 0, keepdims=False)
        key_taken = jnp.take(key_head, listed, axis=0)
        value_taken = jnp.take(value_head, listed, axis=0)
        scores = jnp.einsum("tqd,tjkd->tqjk", query_head.astype(jnp.float32), key_taken.astype(jnp.float32)) * scale
        mask = live_head[:, None, :, None]
        masked = jnp.where(mask, scores, -1e30)
        top = jnp.max(masked, axis=(2, 3), keepdims=True)
        weights = jnp.where(mask, jnp.exp(masked - top), 0.0)
        total = jnp.sum(weights, axis=(2, 3))
        rounded = weights.astype(jnp.bfloat16)
        mixed = jnp.einsum("tqjk,tjkd->tqd", rounded.astype(jnp.float32), value_taken.astype(jnp.float32))
        return (mixed / total[:, :, None]).astype(jnp.bfloat16)

    results = lax.map(one_head, jnp.arange(HEADS, dtype=jnp.int32))
    return results.transpose(1, 2, 0, 3).reshape(tiles * BLOCK, HEADS * HEAD_DIM)
```

```python
import functools

import jax
import jax.numpy as jnp
from jax import lax
from jax.experimental import pallas as pl
from jax.experimental.pallas import tpu as pltpu
from jax.sharding import PartitionSpec as P

HEAD_DIM = 128
BLOCK = 128
LOG2_E = 1.4426950408889634
DEAD = -1e30


def tables(block_lists, block_counts, owner, seq_size):
    heads, tiles, listed = block_lists.shape
    per_index = tiles // seq_size
    lists = lax.dynamic_slice_in_dim(block_lists, owner * per_index, per_index, 1)
    counts = lax.dynamic_slice_in_dim(block_counts, owner * per_index, per_index, 1)
    slot_live = jnp.arange(listed, dtype=jnp.int32) < counts[:, :, None]
    ids = jnp.arange(tiles, dtype=jnp.int32)
    hits = (lists[:, :, :, None] == ids) & slot_live[:, :, :, None]
    keep = jnp.any(hits, axis=2).astype(jnp.int32).reshape(heads, per_index, seq_size, per_index)
    low, high = keep[..., 0], keep[..., 1]
    taken = jnp.max(high, axis=1)
    live = jnp.where(taken[:, None, :] == 1, high, low)
    other = jnp.where(taken[:, None, :] == 1, low, high)
    bits = jnp.array([2 << tile for tile in range(per_index)], jnp.int32)[None, :, None]
    code = taken + jnp.sum(live * bits, axis=1)
    code_other = (1 - taken) + jnp.sum(other * bits, axis=1)
    mine = jnp.arange(seq_size) == owner
    extra = jnp.sum(jnp.where(mine, code_other, 0), axis=1, keepdims=True)
    return jnp.concatenate([code, extra], axis=1)


def attend(query, codes, key_block, value_block):
    rows = query.shape[0]
    factor = HEAD_DIM ** (-0.5) * LOG2_E
    masked = []
    for j, code in enumerate(codes):
        scores = lax.dot_general(
            query, key_block(j, code & 1), (((1,), (1,)), ((), ())), preferred_element_type=jnp.float32
        )
        parts = []
        for tile in range(rows // BLOCK):
            bias = jnp.where((code >> (tile + 1)) & 1 == 1, 0.0, DEAD).astype(jnp.float32)
            parts.append(scores[tile * BLOCK : (tile + 1) * BLOCK] * factor + bias)
        masked.append(jnp.concatenate(parts, axis=0))
    top = jnp.max(functools.reduce(jnp.maximum, masked), axis=1, keepdims=True)
    total, mixed = None, None
    for j, code in enumerate(codes):
        weights = jnp.exp2(masked[j] - top)
        total = weights if total is None else total + weights
        product = jnp.dot(
            weights.astype(jnp.bfloat16), value_block(j, code & 1), preferred_element_type=jnp.float32
        )
        mixed = product if mixed is None else mixed + product
    return mixed / jnp.sum(total, axis=1, keepdims=True)


def gathered_kernel(seq_size, own_rows, info_ref, code_ref, query_ref, key_ref, value_ref, out_ref):
    head = pl.program_id(0)
    owner = info_ref[0]

    def block(ref):
        def read(j, which):
            index = owner if j == seq_size else j
            return ref[pl.ds(pl.multiple_of(index * own_rows + which * BLOCK, BLOCK), BLOCK), :]

        return read

    codes = [code_ref[head * (seq_size + 1) + j] for j in range(seq_size + 1)]
    out_ref[...] = attend(query_ref[...], codes, block(key_ref), block(value_ref)).astype(out_ref.dtype)


def gathered(queries, key_rows, value_rows, block_lists, block_counts, seq_size):
    rows, width = queries.shape
    heads = width // HEAD_DIM
    position = lax.axis_index("seq")
    keys = lax.all_gather(key_rows, "seq", axis=0, tiled=True)
    values = lax.all_gather(value_rows, "seq", axis=0, tiled=True)
    codes = tables(block_lists, block_counts, position, seq_size).reshape(-1)
    all_rows = keys.shape[0]
    out = pl.pallas_call(
        functools.partial(gathered_kernel, seq_size, rows),
        out_shape=jax.ShapeDtypeStruct((rows, width), queries.dtype),
        grid_spec=pltpu.PrefetchScalarGridSpec(
            num_scalar_prefetch=2,
            grid=(heads,),
            in_specs=[
                pl.BlockSpec((rows, HEAD_DIM), lambda h, *_: (0, h)),
                pl.BlockSpec((all_rows, HEAD_DIM), lambda h, *_: (0, h)),
                pl.BlockSpec((all_rows, HEAD_DIM), lambda h, *_: (0, h)),
            ],
            out_specs=pl.BlockSpec((rows, HEAD_DIM), lambda h, *_: (0, h)),
        ),
        name="attend_gathered",
    )(position.reshape(1), codes, queries, keys, values)
    return lax.all_to_all(out, "panel", split_axis=0, concat_axis=1, tiled=True)


def solution(mesh):
    seq_size = mesh.shape["seq"]
    return jax.shard_map(
        functools.partial(gathered, seq_size=seq_size),
        mesh=mesh,
        in_specs=(
            P(("groups", "seq"), "panel"),
            P(("groups", "seq"), "panel"),
            P(("groups", "seq"), "panel"),
            P("panel", None, None),
            P("panel", None),
        ),
        out_specs=P(("groups", "seq", "panel"), None),
        check_vma=False,
    )
```

```python
import functools

import jax
import jax.numpy as jnp
from jax import lax
from jax.experimental import pallas as pl
from jax.experimental.pallas import tpu as pltpu
from jax.sharding import PartitionSpec as P

HEAD_DIM = 128
BLOCK = 128
LOG2_E = 1.4426950408889634
DEAD = -1e30
CORES = 2


def tables(block_lists, block_counts, owner, seq_size):
    heads, tiles, listed = block_lists.shape
    per_index = tiles // seq_size
    lists = lax.dynamic_slice_in_dim(block_lists, owner * per_index, per_index, 1)
    counts = lax.dynamic_slice_in_dim(block_counts, owner * per_index, per_index, 1)
    slot_live = jnp.arange(listed, dtype=jnp.int32) < counts[:, :, None]
    ids = jnp.arange(tiles, dtype=jnp.int32)
    hits = (lists[:, :, :, None] == ids) & slot_live[:, :, :, None]
    keep = jnp.any(hits, axis=2).astype(jnp.int32).reshape(heads, per_index, seq_size, per_index)
    low, high = keep[..., 0], keep[..., 1]
    taken = jnp.max(high, axis=1)
    live = jnp.where(taken[:, None, :] == 1, high, low)
    other = jnp.where(taken[:, None, :] == 1, low, high)
    bits = jnp.array([2 << tile for tile in range(per_index)], jnp.int32)[None, :, None]
    code = taken + jnp.sum(live * bits, axis=1)
    code_other = (1 - taken) + jnp.sum(other * bits, axis=1)
    mine = jnp.arange(seq_size) == owner
    extra = jnp.sum(jnp.where(mine, code_other, 0), axis=1, keepdims=True)
    return jnp.concatenate([code, extra], axis=1)


def attend(query, codes, key_block, value_block):
    rows = query.shape[0]
    factor = HEAD_DIM ** (-0.5) * LOG2_E
    masked = []
    for j, code in enumerate(codes):
        scores = lax.dot_general(
            query, key_block(j, code & 1), (((1,), (1,)), ((), ())), preferred_element_type=jnp.float32
        )
        parts = []
        for tile in range(rows // BLOCK):
            bias = jnp.where((code >> (tile + 1)) & 1 == 1, 0.0, DEAD).astype(jnp.float32)
            parts.append(scores[tile * BLOCK : (tile + 1) * BLOCK] * factor + bias)
        masked.append(jnp.concatenate(parts, axis=0))
    top = jnp.max(functools.reduce(jnp.maximum, masked), axis=1, keepdims=True)
    total, mixed = None, None
    for j, code in enumerate(codes):
        weights = jnp.exp2(masked[j] - top)
        total = weights if total is None else total + weights
        product = jnp.dot(
            weights.astype(jnp.bfloat16), value_block(j, code & 1), preferred_element_type=jnp.float32
        )
        mixed = product if mixed is None else mixed + product
    return mixed / jnp.sum(total, axis=1, keepdims=True)


def gathered_kernel(seq_size, own_rows, info_ref, code_ref, query_ref, key_ref, value_ref, out_ref):
    head = pl.program_id(0)
    owner = info_ref[0]

    def block(ref):
        def read(j, which):
            index = owner if j == seq_size else j
            return ref[pl.ds(pl.multiple_of(index * own_rows + which * BLOCK, BLOCK), BLOCK), :]

        return read

    codes = [code_ref[head * (seq_size + 1) + j] for j in range(seq_size + 1)]
    out_ref[...] = attend(query_ref[...], codes, block(key_ref), block(value_ref)).astype(out_ref.dtype)


def gathered(queries, key_rows, value_rows, block_lists, block_counts, seq_size):
    rows, width = queries.shape
    heads = width // HEAD_DIM
    position = lax.axis_index("seq")
    keys = lax.all_gather(key_rows, "seq", axis=0, tiled=True)
    values = lax.all_gather(value_rows, "seq", axis=0, tiled=True)
    codes = tables(block_lists, block_counts, position, seq_size).reshape(-1)
    all_rows = keys.shape[0]
    out = pl.pallas_call(
        functools.partial(gathered_kernel, seq_size, rows),
        out_shape=jax.ShapeDtypeStruct((rows, width), queries.dtype),
        grid_spec=pltpu.PrefetchScalarGridSpec(
            num_scalar_prefetch=2,
            grid=(heads,),
            in_specs=[
                pl.BlockSpec((rows, HEAD_DIM), lambda h, *_: (0, h)),
                pl.BlockSpec((all_rows, HEAD_DIM), lambda h, *_: (0, h)),
                pl.BlockSpec((all_rows, HEAD_DIM), lambda h, *_: (0, h)),
            ],
            out_specs=pl.BlockSpec((rows, HEAD_DIM), lambda h, *_: (0, h)),
        ),
        name="attend_gathered",
    )(position.reshape(1), codes, queries, keys, values)
    return lax.all_to_all(out, "panel", split_axis=0, concat_axis=1, tiled=True)


def pieces_of(seq_pairs, panel_size, shift):
    return [
        (source * panel_size + panel, target * panel_size + (panel + shift) % panel_size)
        for source, target in seq_pairs
        for panel in range(panel_size)
    ]


def relayed_kernel(seq_size, panel_size, heads, offset, *refs):
    info_ref, code_ref, own_query, guest_query = refs[:4]
    whole = refs[4:12]
    stacked = refs[12:16]
    own_out = refs[16 : 16 + panel_size]
    guest_out = refs[16 + panel_size : 16 + 2 * panel_size]
    held = refs[-1]
    head = pl.program_id(0) + offset
    panel = info_ref[1]
    rows = own_query.shape[0]
    piece = rows // panel_size

    def read(kind, home):
        def block(j, which):
            slot = home if j == seq_size else j
            if slot < 4:
                ref, start = whole[2 * slot + kind], 0
            else:
                ref, start = stacked[slot - 4], kind * rows
            return ref[pl.ds(pl.multiple_of(start + which * BLOCK, BLOCK), BLOCK), :]

        return block

    @pl.when(info_ref[0] == 1)
    def _():
        for side, (query, home, outs) in enumerate(((own_query, 0, own_out), (guest_query, 4, guest_out))):
            first = (side * heads + head) * (seq_size + 1)
            codes = [code_ref[first + j] for j in range(seq_size + 1)]
            held[...] = attend(query[...], codes, read(0, home), read(1, home))
            for shift in range(panel_size):
                start = lax.rem(panel + shift, panel_size) * piece
                outs[shift][...] = held[pl.ds(pl.multiple_of(start, piece), piece), :].astype(outs[shift].dtype)


def assemble_kernel(panel_size, sizes, info_ref, *refs):
    out_ref = refs[-1]
    count = len(sizes)
    width = out_ref.shape[1] // panel_size
    panel = info_ref[1]
    inner = info_ref[0] == 1
    for shift in range(panel_size):
        source = lax.rem(panel + panel_size - shift, panel_size)
        start = 0
        for chunk, size in enumerate(sizes):
            own = refs[chunk * panel_size + shift]
            guest = refs[(count + chunk) * panel_size + shift]
            columns = pl.ds(pl.multiple_of(source * width + start, HEAD_DIM), size * HEAD_DIM)

            @pl.when(inner)
            def _():
                out_ref[:, columns] = own[...]

            @pl.when(jnp.logical_not(inner))
            def _():
                out_ref[:, columns] = guest[...]

            start += size * HEAD_DIM


def chunk_sizes(heads):
    sizes, left = [], heads
    while left > 1:
        size = -(-left // 2) if left <= 3 else -(-left * 2 // 5)
        sizes.append(size)
        left -= size
    return sizes + [1] * left


def relayed(queries, key_rows, value_rows, block_lists, block_counts, seq_size, panel_size):
    rows, width = queries.shape
    heads = width // HEAD_DIM
    chips = seq_size // CORES
    position = lax.axis_index("seq")
    panel = lax.axis_index("panel")
    chip, core = position // CORES, position % CORES
    last = chips - 1
    cores = range(CORES)
    inward = [(source * CORES + c, target * CORES + c) for source, target in ((0, 1), (last, last - 1)) for c in cores]
    across = [(source * CORES + c, target * CORES + c) for source, target in ((1, 2), (2, 1)) for c in cores]
    partner = [(z * CORES + c, z * CORES + CORES - 1 - c) for z in (1, 2) for c in cores]
    inner = [(z * CORES + c, z * CORES + c) for z in (1, 2) for c in cores]
    outward = [(target, source) for source, target in inward]

    sizes = chunk_sizes(heads)
    starts = [sum(sizes[:k]) for k in range(len(sizes))]
    permute = lambda x, pairs: lax.ppermute(x, "seq", pairs)
    middle = [permute(x, across) for x in (key_rows, value_rows)]
    guest_query = permute(queries, inward)
    ends, far = [], []
    for start, size in zip(starts, sizes):
        columns = slice(start * HEAD_DIM, (start + size) * HEAD_DIM)
        ends.append(permute(jnp.concatenate([key_rows[:, columns], value_rows[:, columns]], axis=0), inward))
        far.append(permute(ends[-1], across))
    beside = [permute(x, partner) for x in (key_rows, value_rows)]
    middle_beside = [permute(x, partner) for x in middle]

    is_inner = (chip >= 1) & (chip < last)
    end = jnp.where(chip * 2 < chips, 0, last)
    guest = end * CORES + core
    order = jnp.stack(
        [
            z * CORES + c
            for z in (chip, last - chip, end, last - end)
            for c in (core, CORES - 1 - core)
        ]
    )
    pick = (order[:, None] == jnp.arange(seq_size)).astype(jnp.int32)

    def arranged(owner):
        codes = tables(block_lists, block_counts, owner, seq_size)
        return jnp.concatenate([jnp.sum(codes[:, None, :seq_size] * pick, axis=2), codes[:, seq_size:]], axis=1)

    codes = jnp.stack([arranged(position), arranged(guest)]).reshape(-1)
    info = jnp.stack([is_inner.astype(jnp.int32), panel])

    own_pieces, guest_pieces = [], []
    for k, (start, size) in enumerate(zip(starts, sizes)):
        stacked = [ends[k], permute(ends[k], partner), far[k], permute(far[k], partner)]
        at = lambda h, *_, start=start: (0, h + start)
        whole = [pl.BlockSpec((rows, HEAD_DIM), at)] * 10
        part = [pl.BlockSpec((2 * rows, HEAD_DIM), lambda h, *_: (0, h))] * 4
        outs = pl.pallas_call(
            functools.partial(relayed_kernel, seq_size, panel_size, heads, start),
            out_shape=[jax.ShapeDtypeStruct((rows // panel_size, size * HEAD_DIM), queries.dtype)] * (2 * panel_size),
            grid_spec=pltpu.PrefetchScalarGridSpec(
                num_scalar_prefetch=2,
                grid=(size,),
                in_specs=whole + part,
                out_specs=[pl.BlockSpec((rows // panel_size, HEAD_DIM), lambda h, *_: (0, h))] * (2 * panel_size),
                scratch_shapes=[pltpu.VMEM((rows, HEAD_DIM), jnp.float32)],
            ),
            cost_estimate=pl.CostEstimate(
                flops=size * 8 * rows * (seq_size + 1) * BLOCK * HEAD_DIM,
                bytes_accessed=size * HEAD_DIM * 2 * rows * 20,
                transcendentals=size * 2 * rows * (seq_size + 1) * BLOCK,
            ),
            name="attend_%d" % k,
        )(info, codes, queries, guest_query, key_rows, value_rows, *beside, *middle, *middle_beside, *stacked)
        both = ("seq", "panel")
        for shift in range(panel_size):
            mine, theirs = outs[shift], outs[panel_size + shift]
            own_pieces.append(mine if shift == 0 else lax.ppermute(mine, both, pieces_of(inner, panel_size, shift)))
            guest_pieces.append(lax.ppermute(theirs, both, pieces_of(outward, panel_size, shift)))

    return pl.pallas_call(
        functools.partial(assemble_kernel, panel_size, sizes),
        out_shape=jax.ShapeDtypeStruct((rows // panel_size, width * panel_size), queries.dtype),
        in_specs=[pl.BlockSpec(memory_space=pltpu.SMEM)]
        + [pl.BlockSpec(memory_space=pltpu.VMEM)] * (len(own_pieces) + len(guest_pieces)),
        out_specs=pl.BlockSpec(memory_space=pltpu.VMEM),
        name="assemble",
    )(info, *own_pieces, *guest_pieces)


def solution(mesh):
    seq_size, panel_size = mesh.shape["seq"], mesh.shape["panel"]
    if seq_size // CORES - 2 == 2:
        body = functools.partial(relayed, seq_size=seq_size, panel_size=panel_size)
    else:
        body = functools.partial(gathered, seq_size=seq_size)
    return jax.shard_map(
        body,
        mesh=mesh,
        in_specs=(
            P(("groups", "seq"), "panel"),
            P(("groups", "seq"), "panel"),
            P(("groups", "seq"), "panel"),
            P("panel", None, None),
            P("panel", None),
        ),
        out_specs=P(("groups", "seq", "panel"), None),
        check_vma=False,
    )
```

```python
import functools

import jax
import jax.numpy as jnp
from jax import lax
from jax.experimental import pallas as pl
from jax.experimental.pallas import tpu as pltpu
from jax.sharding import PartitionSpec as P


HEAD_DIM = 128
BLOCK = 128
LOG2_E = 1.4426950408889634
DEAD = -1e30
CORES = 2
CHUNKS = 3
VMEM_GRANT = 12 << 20


def tables(block_lists, block_counts, owner, seq_size):
    heads, tiles, listed = block_lists.shape
    per_index = tiles // seq_size
    lists = lax.dynamic_slice_in_dim(block_lists, owner * per_index, per_index, 1)
    counts = lax.dynamic_slice_in_dim(block_counts, owner * per_index, per_index, 1)
    slot_live = jnp.arange(listed, dtype=jnp.int32) < counts[:, :, None]
    ids = jnp.arange(tiles, dtype=jnp.int32)
    hits = (lists[:, :, :, None] == ids) & slot_live[:, :, :, None]
    keep = jnp.any(hits, axis=2).astype(jnp.int32).reshape(heads, per_index, seq_size, per_index)
    low, high = keep[..., 0], keep[..., 1]
    taken = jnp.max(high, axis=1)
    live = jnp.where(taken[:, None, :] == 1, high, low)
    other = jnp.where(taken[:, None, :] == 1, low, high)
    bits = jnp.array([2 << tile for tile in range(per_index)], jnp.int32)[None, :, None]
    code = taken + jnp.sum(live * bits, axis=1)
    code_other = (1 - taken) + jnp.sum(other * bits, axis=1)
    mine = jnp.arange(seq_size) == owner
    extra = jnp.sum(jnp.where(mine, code_other, 0), axis=1, keepdims=True)
    return jnp.concatenate([code, extra], axis=1)


def attend(query, codes, key_block, value_block):
    rows = query.shape[0]
    factor = HEAD_DIM ** (-0.5) * LOG2_E
    masked = []
    for j, code in enumerate(codes):
        scores = lax.dot_general(
            query, key_block(j, code & 1), (((1,), (1,)), ((), ())), preferred_element_type=jnp.float32
        )
        parts = []
        for tile in range(rows // BLOCK):
            bias = jnp.where((code >> (tile + 1)) & 1 == 1, 0.0, DEAD).astype(jnp.float32)
            parts.append(scores[tile * BLOCK : (tile + 1) * BLOCK] * factor + bias)
        masked.append(jnp.concatenate(parts, axis=0))
    top = jnp.max(functools.reduce(jnp.maximum, masked), axis=1, keepdims=True)
    total, mixed = None, None
    for j, code in enumerate(codes):
        weights = jnp.exp2(masked[j] - top)
        total = weights if total is None else total + weights
        product = jnp.dot(
            weights.astype(jnp.bfloat16), value_block(j, code & 1), preferred_element_type=jnp.float32
        )
        mixed = product if mixed is None else mixed + product
    return mixed / jnp.sum(total, axis=1, keepdims=True)


def gathered_kernel(seq_size, own_rows, info_ref, code_ref, query_ref, key_ref, value_ref, out_ref):
    head = pl.program_id(0)
    owner = info_ref[0]

    def block(ref):
        def read(j, which):
            index = owner if j == seq_size else j
            return ref[pl.ds(pl.multiple_of(index * own_rows + which * BLOCK, BLOCK), BLOCK), :]

        return read

    codes = [code_ref[head * (seq_size + 1) + j] for j in range(seq_size + 1)]
    out_ref[...] = attend(query_ref[...], codes, block(key_ref), block(value_ref)).astype(out_ref.dtype)


def gathered(queries, key_rows, value_rows, block_lists, block_counts, seq_size):
    rows, width = queries.shape
    heads = width // HEAD_DIM
    position = lax.axis_index("seq")
    keys = lax.all_gather(key_rows, "seq", axis=0, tiled=True)
    values = lax.all_gather(value_rows, "seq", axis=0, tiled=True)
    codes = tables(block_lists, block_counts, position, seq_size).reshape(-1)
    all_rows = keys.shape[0]
    out = pl.pallas_call(
        functools.partial(gathered_kernel, seq_size, rows),
        out_shape=jax.ShapeDtypeStruct((rows, width), queries.dtype),
        grid_spec=pltpu.PrefetchScalarGridSpec(
            num_scalar_prefetch=2,
            grid=(heads,),
            in_specs=[
                pl.BlockSpec((rows, HEAD_DIM), lambda h, *_: (0, h)),
                pl.BlockSpec((all_rows, HEAD_DIM), lambda h, *_: (0, h)),
                pl.BlockSpec((all_rows, HEAD_DIM), lambda h, *_: (0, h)),
            ],
            out_specs=pl.BlockSpec((rows, HEAD_DIM), lambda h, *_: (0, h)),
        ),
        name="attend_gathered",
    )(position.reshape(1), codes, queries, keys, values)
    return lax.all_to_all(out, "panel", split_axis=0, concat_axis=1, tiled=True)


def pieces_of(seq_pairs, panel_size, shift):
    return [
        (source * panel_size + panel, target * panel_size + (panel + shift) % panel_size)
        for source, target in seq_pairs
        for panel in range(panel_size)
    ]


def send(value, pairs, axes="seq"):
    return lax.ppermute(value, axes, pairs)


def pack_kernel(starts, sizes, key_ref, value_ref, *refs):
    outs, sems = refs[:-1], refs[-1]
    rows = key_ref.shape[0]
    copies = []
    for k, (start, size) in enumerate(zip(starts, sizes)):
        columns = pl.ds(start * HEAD_DIM, size * HEAD_DIM)
        for kind, ref in enumerate((key_ref, value_ref)):
            copies.append(
                pltpu.make_async_copy(ref.at[:, columns], outs[k].at[pl.ds(kind * rows, rows), :], sems.at[k, kind])
            )
            copies[-1].start()
    for copy in copies:
        copy.wait()


def relayed_kernel(seq_size, panel_size, heads, start, size, *refs):
    info_ref, code_ref, own_query, guest_query = refs[:4]
    whole = refs[4:10]
    stacked = refs[10:15]
    own_out = refs[15 : 15 + panel_size]
    guest_out = refs[15 + panel_size : 15 + 2 * panel_size]
    held = refs[-1]
    panel = info_ref[1]
    rows = own_query.shape[0]
    piece = rows // panel_size

    def unit(h, side, spot):
        query, home, outs = ((own_query, 0, own_out), (guest_query, 4, guest_out))[side]
        local = pl.ds(pl.multiple_of(h * HEAD_DIM, HEAD_DIM), HEAD_DIM)
        full = pl.ds(pl.multiple_of((h + start) * HEAD_DIM, HEAD_DIM), HEAD_DIM)

        def read(kind):
            def block(j, which):
                slot = home if j == seq_size else j
                if 1 <= slot <= 3:
                    ref, first, columns = whole[2 * (slot - 1) + kind], 0, full
                else:
                    ref, first, columns = stacked[slot - 3 if slot else 0], kind * rows, local
                return ref[pl.ds(pl.multiple_of(first + which * BLOCK, BLOCK), BLOCK), columns]

            return block

        first = (side * heads + h + start) * (seq_size + 1)
        codes = [code_ref[first + j] for j in range(seq_size + 1)]
        result = attend(query[:, full], codes, read(0), read(1))
        held[spot] = result
        for shift in range(panel_size):
            first_row = pl.multiple_of(lax.rem(panel + shift, panel_size) * piece, piece)
            outs[shift][:, local] = held[spot, pl.ds(first_row, piece), :].astype(outs[shift].dtype)

    @pl.when(info_ref[0] == 1)
    def _():
        if size > 1:

            @pl.loop(0, size // 2)
            def _(pair):
                for h in range(2):
                    for side in range(2):
                        unit(pair * 2 + h, side, h * 2 + side)

        for h in range(size - size % 2, size):
            for side in range(2):
                unit(h, side, side)


def assemble_kernel(panel_size, starts, sizes, aliased, info_ref, *refs):
    out_ref, sems = refs[-2:]
    refs = refs[1:] if aliased else refs
    count = len(sizes)
    width = out_ref.shape[1] // panel_size
    panel = info_ref[1]
    inner = info_ref[0] == 1
    copies = []
    for shift in range(panel_size):
        source = lax.rem(panel + panel_size - shift, panel_size)
        for chunk, (start, size) in enumerate(zip(starts, sizes)):
            columns = pl.ds(pl.multiple_of(source * width + start * HEAD_DIM, HEAD_DIM), size * HEAD_DIM)
            own, guest = (
                pltpu.make_async_copy(
                    refs[(side * count + chunk) * panel_size + shift],
                    out_ref.at[:, columns],
                    sems.at[shift, chunk],
                )
                for side in range(2)
            )
            pl.when(inner)(own.start)
            pl.when(jnp.logical_not(inner))(guest.start)
            copies.append(own)
    for copy in copies:
        copy.wait()


def relayed(queries, key_rows, value_rows, block_lists, block_counts, seq_size, panel_size):
    rows, width = queries.shape
    heads = width // HEAD_DIM
    chips = seq_size // CORES
    position = lax.axis_index("seq")
    panel = lax.axis_index("panel")
    chip, core = position // CORES, position % CORES
    last = chips - 1
    cores = range(CORES)
    inward = [(source * CORES + c, target * CORES + c) for source, target in ((0, 1), (last, last - 1)) for c in cores]
    across = [(source * CORES + c, target * CORES + c) for source, target in ((1, 2), (2, 1)) for c in cores]
    partner = [(z * CORES + c, z * CORES + CORES - 1 - c) for z in (1, 2) for c in cores]
    inner = [(z * CORES + c, z * CORES + c) for z in (1, 2) for c in cores]
    outward = [(target, source) for source, target in inward]
    in_vmem, in_smem, anywhere = (pl.BlockSpec(memory_space=s) for s in (pltpu.VMEM, pltpu.SMEM, pl.ANY))

    chunks = min(CHUNKS, heads)
    starts = [heads * k // chunks for k in range(chunks)]
    sizes = [heads * (k + 1) // chunks - heads * k // chunks for k in range(chunks)]

    middle = [send(x, across) for x in (key_rows, value_rows)]
    packed = pl.pallas_call(
        functools.partial(pack_kernel, starts, sizes),
        out_shape=[jax.ShapeDtypeStruct((2 * rows, size * HEAD_DIM), key_rows.dtype) for size in sizes],
        in_specs=[anywhere] * 2,
        out_specs=[in_vmem] * chunks,
        scratch_shapes=[pltpu.SemaphoreType.DMA((chunks, 2))],
        compiler_params=pltpu.CompilerParams(vmem_limit_bytes=VMEM_GRANT),
        name="pack",
    )(key_rows, value_rows)
    beside = [send(x, partner) for x in (key_rows, value_rows)]
    ends = [send(x, inward) for x in packed]
    guest_query = send(queries, inward)
    middle_beside = [send(x, partner) for x in middle]

    is_inner = (chip >= 1) & (chip < last)
    end = jnp.where(chip * 2 < chips, 0, last)
    guest = end * CORES + core
    order = jnp.stack(
        [
            z * CORES + c
            for z in (chip, last - chip, end, last - end)
            for c in (core, CORES - 1 - core)
        ]
    )
    pick = (order[:, None] == jnp.arange(seq_size)).astype(jnp.int32)

    def arranged(owner):
        codes = tables(block_lists, block_counts, owner, seq_size)
        return jnp.concatenate([jnp.sum(codes[:, None, :seq_size] * pick, axis=2), codes[:, seq_size:]], axis=1)

    codes = jnp.stack([arranged(position), arranged(guest)]).reshape(-1)
    info = jnp.stack([is_inner.astype(jnp.int32), panel])

    own_pieces, guest_pieces = [], []
    for k, (start, size) in enumerate(zip(starts, sizes)):
        far = send(ends[k], across)
        ends_beside = send(ends[k], partner)
        far_beside = send(far, partner)
        stacked = [packed[k], ends[k], ends_beside, far, far_beside]
        outs = pl.pallas_call(
            functools.partial(relayed_kernel, seq_size, panel_size, heads, start, size),
            out_shape=[jax.ShapeDtypeStruct((rows // panel_size, size * HEAD_DIM), queries.dtype)] * (2 * panel_size),
            in_specs=[in_smem] * 2 + [in_vmem] * 13,
            out_specs=[in_vmem] * (2 * panel_size),
            scratch_shapes=[pltpu.VMEM((4, rows, HEAD_DIM), jnp.float32)],
            compiler_params=pltpu.CompilerParams(vmem_limit_bytes=VMEM_GRANT),
            cost_estimate=pl.CostEstimate(
                flops=size * 8 * rows * (seq_size + 1) * BLOCK * HEAD_DIM,
                bytes_accessed=size * HEAD_DIM * 2 * rows * 20,
                transcendentals=size * 2 * rows * (seq_size + 1) * BLOCK,
            ),
        )(info, codes, queries, guest_query, *beside, *middle, *middle_beside, *stacked)
        both = ("seq", "panel")
        for shift in range(panel_size):
            mine, theirs = outs[shift], outs[panel_size + shift]
            if shift:
                mine = send(mine, pieces_of(inner, panel_size, shift), both)
            own_pieces.append(mine)
            guest_pieces.append(send(theirs, pieces_of(outward, panel_size, shift), both))

    split = (chunks - 1) * panel_size
    out = None
    for lo, hi, first, final in ((0, split, 0, chunks - 1), (split, chunks * panel_size, chunks - 1, chunks)):
        if lo == hi:
            continue
        pieces = own_pieces[lo:hi] + guest_pieces[lo:hi]
        before = [] if out is None else [out]
        out = pl.pallas_call(
            functools.partial(assemble_kernel, panel_size, starts[first:final], sizes[first:final], len(before)),
            out_shape=jax.ShapeDtypeStruct((rows // panel_size, width * panel_size), queries.dtype),
            in_specs=[in_smem] + [anywhere] * len(before) + [in_vmem] * len(pieces),
            out_specs=anywhere,
            scratch_shapes=[pltpu.SemaphoreType.DMA((panel_size, final - first))],
            input_output_aliases={1: 0} if before else {},
            compiler_params=pltpu.CompilerParams(vmem_limit_bytes=VMEM_GRANT),
        )(info, *before, *pieces)
    return out


def solution(mesh):
    seq_size, panel_size = mesh.shape["seq"], mesh.shape["panel"]
    relay = seq_size // CORES - 2 == 2
    if relay:
        body = functools.partial(relayed, seq_size=seq_size, panel_size=panel_size)
    else:
        body = functools.partial(gathered, seq_size=seq_size)
    return jax.shard_map(
        body,
        mesh=mesh,
        in_specs=(
            P(("groups", "seq"), "panel"),
            P(("groups", "seq"), "panel"),
            P(("groups", "seq"), "panel"),
            P("panel", None, None),
            P("panel", None),
        ),
        out_specs=P(("groups", "seq", "panel"), None),
        check_vma=False,
    )
```

```python
import functools

import jax
import jax.numpy as jnp
from jax import lax
from jax.experimental import pallas as pl
from jax.experimental.pallas import tpu as pltpu
from jax.sharding import PartitionSpec as P


HEAD_DIM = 128
BLOCK = 128
LOG2_E = 1.4426950408889634
DEAD = -1e30
CORES = 2
FIRST_SHARE = 7, 12
VMEM_GRANT = 20 << 20


def tables(block_lists, block_counts, owner, seq_size):
    heads, tiles, listed = block_lists.shape
    per_index = tiles // seq_size
    lists = lax.dynamic_slice_in_dim(block_lists, owner * per_index, per_index, 1)
    counts = lax.dynamic_slice_in_dim(block_counts, owner * per_index, per_index, 1)
    slot_live = jnp.arange(listed, dtype=jnp.int32) < counts[:, :, None]
    ids = jnp.arange(tiles, dtype=jnp.int32)
    hits = (lists[:, :, :, None] == ids) & slot_live[:, :, :, None]
    keep = jnp.any(hits, axis=2).astype(jnp.int32).reshape(heads, per_index, seq_size, per_index)
    low, high = keep[..., 0], keep[..., 1]
    taken = jnp.max(high, axis=1)
    live = jnp.where(taken[:, None, :] == 1, high, low)
    other = jnp.where(taken[:, None, :] == 1, low, high)
    bits = jnp.array([2 << tile for tile in range(per_index)], jnp.int32)[None, :, None]
    code = taken + jnp.sum(live * bits, axis=1)
    code_other = (1 - taken) + jnp.sum(other * bits, axis=1)
    mine = jnp.arange(seq_size) == owner
    extra = jnp.sum(jnp.where(mine, code_other, 0), axis=1, keepdims=True)
    return jnp.concatenate([code, extra], axis=1)


def attend(query, codes, key_block, value_block):
    rows = query.shape[0]
    factor = HEAD_DIM ** (-0.5) * LOG2_E
    masked = []
    for j, code in enumerate(codes):
        scores = lax.dot_general(
            query, key_block(j, code & 1), (((1,), (1,)), ((), ())), preferred_element_type=jnp.float32
        )
        parts = []
        for tile in range(rows // BLOCK):
            bias = jnp.where((code >> (tile + 1)) & 1 == 1, 0.0, DEAD).astype(jnp.float32)
            parts.append(scores[tile * BLOCK : (tile + 1) * BLOCK] * factor + bias)
        masked.append(jnp.concatenate(parts, axis=0))
    top = jnp.max(functools.reduce(jnp.maximum, masked), axis=1, keepdims=True)
    total, mixed = None, None
    for j, code in enumerate(codes):
        weights = jnp.exp2(masked[j] - top)
        total = weights if total is None else total + weights
        product = jnp.dot(
            weights.astype(jnp.bfloat16), value_block(j, code & 1), preferred_element_type=jnp.float32
        )
        mixed = product if mixed is None else mixed + product
    return mixed / jnp.sum(total, axis=1, keepdims=True)


def gathered_kernel(seq_size, own_rows, info_ref, code_ref, query_ref, key_ref, value_ref, out_ref):
    head = pl.program_id(0)
    owner = info_ref[0]

    def block(ref):
        def read(j, which):
            index = owner if j == seq_size else j
            return ref[pl.ds(pl.multiple_of(index * own_rows + which * BLOCK, BLOCK), BLOCK), :]

        return read

    codes = [code_ref[head * (seq_size + 1) + j] for j in range(seq_size + 1)]
    out_ref[...] = attend(query_ref[...], codes, block(key_ref), block(value_ref)).astype(out_ref.dtype)


def gathered(queries, key_rows, value_rows, block_lists, block_counts, seq_size):
    rows, width = queries.shape
    heads = width // HEAD_DIM
    position = lax.axis_index("seq")
    keys = lax.all_gather(key_rows, "seq", axis=0, tiled=True)
    values = lax.all_gather(value_rows, "seq", axis=0, tiled=True)
    codes = tables(block_lists, block_counts, position, seq_size).reshape(-1)
    all_rows = keys.shape[0]
    out = pl.pallas_call(
        functools.partial(gathered_kernel, seq_size, rows),
        out_shape=jax.ShapeDtypeStruct((rows, width), queries.dtype),
        grid_spec=pltpu.PrefetchScalarGridSpec(
            num_scalar_prefetch=2,
            grid=(heads,),
            in_specs=[
                pl.BlockSpec((rows, HEAD_DIM), lambda h, *_: (0, h)),
                pl.BlockSpec((all_rows, HEAD_DIM), lambda h, *_: (0, h)),
                pl.BlockSpec((all_rows, HEAD_DIM), lambda h, *_: (0, h)),
            ],
            out_specs=pl.BlockSpec((rows, HEAD_DIM), lambda h, *_: (0, h)),
        ),
        name="attend_gathered",
    )(position.reshape(1), codes, queries, keys, values)
    return lax.all_to_all(out, "panel", split_axis=0, concat_axis=1, tiled=True)


def pieces_of(seq_pairs, panel_size, shift):
    return [
        (source * panel_size + panel, target * panel_size + (panel + shift) % panel_size)
        for source, target in seq_pairs
        for panel in range(panel_size)
    ]


def send(value, pairs, axes="seq"):
    return lax.ppermute(value, axes, pairs)


def pack_kernel(starts, sizes, key_ref, value_ref, *refs):
    outs, sems = refs[:-1], refs[-1]
    rows = key_ref.shape[0]
    copies = []
    for k, (start, size) in enumerate(zip(starts, sizes)):
        columns = pl.ds(start * HEAD_DIM, size * HEAD_DIM)
        for kind, ref in enumerate((key_ref, value_ref)):
            copies.append(
                pltpu.make_async_copy(ref.at[:, columns], outs[k].at[pl.ds(kind * rows, rows), :], sems.at[k, kind])
            )
            copies[-1].start()
    for copy in copies:
        copy.wait()


def masked_scores(query, codes, key_block):
    factor = HEAD_DIM ** (-0.5) * LOG2_E
    masked = []
    for j, code in codes:
        scores = lax.dot_general(
            key_block(j, code & 1), query, (((1,), (1,)), ((), ())), preferred_element_type=jnp.float32
        )
        tiles = query.shape[0] // BLOCK
        bias = [
            jnp.full((1, BLOCK), jnp.where((code >> (tile + 1)) & 1 == 1, 0.0, DEAD), jnp.float32)
            for tile in range(tiles)
        ]
        masked.append(scores * factor + jnp.concatenate(bias, axis=1))
    return masked


def weigh(masked, top, codes, value_block):
    total, mixed = None, None
    for scores, (j, code) in zip(masked, codes):
        weights = jnp.exp2(scores - top)
        total = weights if total is None else total + weights
        product = lax.dot_general(
            value_block(j, code & 1),
            weights.astype(jnp.bfloat16),
            (((0,), (0,)), ((), ())),
            preferred_element_type=jnp.float32,
        )
        mixed = product if mixed is None else mixed + product
    return jnp.sum(total, axis=0, keepdims=True), mixed


def highest(masked):
    return jnp.max(functools.reduce(jnp.maximum, masked), axis=0, keepdims=True)


def each_unit(size, unit):
    @pl.loop(0, size // 2)
    def _(pair):
        for h in range(2):
            for side in range(2):
                unit(pair * 2 + h, side)

    for h in range(size - size % 2, size):
        for side in range(2):
            unit(h, side)


def columns_of(head):
    return pl.ds(pl.multiple_of(head * HEAD_DIM, HEAD_DIM), HEAD_DIM)


def block_reader(pick):
    def block(slot, which):
        ref, first, columns = pick(slot)
        return ref[pl.ds(pl.multiple_of(first + which * BLOCK, BLOCK), BLOCK), columns]

    return block


def early_kernel(seq_size, heads, starts, sizes, *refs):
    info_ref, code_ref = refs[:2]
    queries = refs[2:4]
    whole = refs[4:12]
    sums, stats = refs[12 : 12 + len(sizes)], refs[12 + len(sizes) :]

    @pl.when(info_ref[0] == 1)
    def _():
        for k, (start, size) in enumerate(zip(starts, sizes)):

            def unit(h, side):
                columns = columns_of(h + start)
                first = (side * heads + h + start) * (seq_size + 1)
                codes = [(slot, code_ref[first + slot]) for slot in range(4)]
                if side == 0:
                    codes.append((0, code_ref[first + seq_size]))
                masked = masked_scores(
                    queries[side][:, columns], codes, block_reader(lambda slot: (whole[2 * slot], 0, columns))
                )
                top = highest(masked)
                total, mixed = weigh(
                    masked, top, codes, block_reader(lambda slot: (whole[2 * slot + 1], 0, columns))
                )
                sums[k][h * 2 + side] = mixed
                stats[k][h * 2 + side, pl.ds(0, 1), :] = top
                stats[k][h * 2 + side, pl.ds(1, 1), :] = total

            each_unit(size, unit)


def late_kernel(seq_size, panel_size, heads, start, size, *refs):
    info_ref, code_ref = refs[:2]
    queries = refs[2:4]
    sums, stats = refs[4:6]
    stacked = refs[6:10]
    outs = refs[10 : 10 + panel_size], refs[10 + panel_size : 10 + 2 * panel_size]
    held = refs[-1]
    panel = info_ref[1]
    rows = queries[0].shape[0]
    piece = rows // panel_size

    def unit(h, side):
        local = columns_of(h)
        first = (side * heads + h + start) * (seq_size + 1)
        codes = [(slot, code_ref[first + slot]) for slot in range(4, seq_size)]
        if side == 1:
            codes.append((4, code_ref[first + seq_size]))
        read = lambda kind: block_reader(lambda slot: (stacked[slot - 4], kind * rows, local))
        masked = masked_scores(queries[side][:, columns_of(h + start)], codes, read(0))
        before = stats[h * 2 + side, pl.ds(0, 1), :]
        top = jnp.maximum(before, highest(masked))
        kept = jnp.exp2(before - top)
        total, mixed = weigh(masked, top, codes, read(1))
        total = total + kept * stats[h * 2 + side, pl.ds(1, 1), :]
        mixed = mixed + kept * sums[h * 2 + side]
        spot = (h % 2) * 2 + side
        held[spot] = (mixed / total).T
        for shift in range(panel_size):
            first_row = pl.multiple_of(lax.rem(panel + shift, panel_size) * piece, piece)
            outs[side][shift][:, local] = held[spot, pl.ds(first_row, piece), :].astype(outs[side][shift].dtype)

    @pl.when(info_ref[0] == 1)
    def _():
        each_unit(size, unit)


def assemble_kernel(panel_size, starts, sizes, aliased, info_ref, *refs):
    out_ref, sems = refs[-2:]
    refs = refs[1:] if aliased else refs
    count = len(sizes)
    width = out_ref.shape[1] // panel_size
    panel = info_ref[1]
    inner = info_ref[0] == 1
    copies = []
    for shift in range(panel_size):
        source = lax.rem(panel + panel_size - shift, panel_size)
        for chunk, (start, size) in enumerate(zip(starts, sizes)):
            columns = pl.ds(pl.multiple_of(source * width + start * HEAD_DIM, HEAD_DIM), size * HEAD_DIM)
            own, guest = (
                pltpu.make_async_copy(
                    refs[(side * count + chunk) * panel_size + shift],
                    out_ref.at[:, columns],
                    sems.at[shift, chunk],
                )
                for side in range(2)
            )
            pl.when(inner)(own.start)
            pl.when(jnp.logical_not(inner))(guest.start)
            copies.append(own)
    for copy in copies:
        copy.wait()


def relayed(queries, key_rows, value_rows, block_lists, block_counts, seq_size, panel_size):
    rows, width = queries.shape
    heads = width // HEAD_DIM
    chips = seq_size // CORES
    position = lax.axis_index("seq")
    panel = lax.axis_index("panel")
    chip, core = position // CORES, position % CORES
    last = chips - 1
    cores = range(CORES)
    inward = [(source * CORES + c, target * CORES + c) for source, target in ((0, 1), (last, last - 1)) for c in cores]
    across = [(source * CORES + c, target * CORES + c) for source, target in ((1, 2), (2, 1)) for c in cores]
    partner = [(z * CORES + c, z * CORES + CORES - 1 - c) for z in (1, 2) for c in cores]
    inner = [(z * CORES + c, z * CORES + c) for z in (1, 2) for c in cores]
    outward = [(target, source) for source, target in inward]
    in_vmem, in_smem, anywhere = (pl.BlockSpec(memory_space=s) for s in (pltpu.VMEM, pltpu.SMEM, pl.ANY))

    front = max(1, heads * FIRST_SHARE[0] // FIRST_SHARE[1])
    sizes = [front, heads - front]
    starts = [0, front]
    chunks = len(sizes)

    middle = [send(x, across) for x in (key_rows, value_rows)]
    packed = pl.pallas_call(
        functools.partial(pack_kernel, starts, sizes),
        out_shape=[jax.ShapeDtypeStruct((2 * rows, size * HEAD_DIM), key_rows.dtype) for size in sizes],
        in_specs=[anywhere] * 2,
        out_specs=[in_vmem] * chunks,
        scratch_shapes=[pltpu.SemaphoreType.DMA((chunks, 2))],
        compiler_params=pltpu.CompilerParams(vmem_limit_bytes=VMEM_GRANT),
        name="pack",
    )(key_rows, value_rows)
    beside = [send(x, partner) for x in (key_rows, value_rows)]
    ends = [send(x, inward) for x in packed]
    guest_query = send(queries, inward)
    middle_beside = [send(x, partner) for x in middle]

    is_inner = (chip >= 1) & (chip < last)
    end = jnp.where(chip * 2 < chips, 0, last)
    guest = end * CORES + core
    order = jnp.stack(
        [
            z * CORES + c
            for z in (chip, last - chip, end, last - end)
            for c in (core, CORES - 1 - core)
        ]
    )
    pick = (order[:, None] == jnp.arange(seq_size)).astype(jnp.int32)

    def arranged(owner):
        codes = tables(block_lists, block_counts, owner, seq_size)
        return jnp.concatenate([jnp.sum(codes[:, None, :seq_size] * pick, axis=2), codes[:, seq_size:]], axis=1)

    codes = jnp.stack([arranged(position), arranged(guest)]).reshape(-1)
    info = jnp.stack([is_inner.astype(jnp.int32), panel])

    units = [2 * size for size in sizes]
    params = pltpu.CompilerParams(vmem_limit_bytes=VMEM_GRANT)
    cost = lambda count, blocks: pl.CostEstimate(
        flops=count * 4 * rows * blocks * BLOCK * HEAD_DIM,
        bytes_accessed=count * blocks * 4 * BLOCK * HEAD_DIM,
        transcendentals=count * rows * blocks * BLOCK,
    )
    state = pl.pallas_call(
        functools.partial(early_kernel, seq_size, heads, starts, sizes),
        out_shape=[jax.ShapeDtypeStruct((count, HEAD_DIM, rows), jnp.float32) for count in units]
        + [jax.ShapeDtypeStruct((count, 8, rows), jnp.float32) for count in units],
        in_specs=[in_smem] * 2 + [in_vmem] * 10,
        out_specs=[in_vmem] * (2 * chunks),
        compiler_params=params,
        cost_estimate=cost(2 * heads, 5),
        name="early",
    )(info, codes, queries, guest_query, key_rows, value_rows, *beside, *middle, *middle_beside)

    own_pieces, guest_pieces = [], []
    for k, (start, size) in enumerate(zip(starts, sizes)):
        far = send(ends[k], across)
        ends_beside = send(ends[k], partner)
        far_beside = send(far, partner)
        outs = pl.pallas_call(
            functools.partial(late_kernel, seq_size, panel_size, heads, start, size),
            out_shape=[jax.ShapeDtypeStruct((rows // panel_size, size * HEAD_DIM), queries.dtype)] * (2 * panel_size),
            in_specs=[in_smem] * 2 + [in_vmem] * 8,
            out_specs=[in_vmem] * (2 * panel_size),
            scratch_shapes=[pltpu.VMEM((4, rows, HEAD_DIM), jnp.float32)],
            compiler_params=params,
            cost_estimate=cost(2 * size, 5),
        )(info, codes, queries, guest_query, state[k], state[chunks + k], ends[k], ends_beside, far, far_beside)
        both = ("seq", "panel")
        for shift in range(panel_size):
            mine, theirs = outs[shift], outs[panel_size + shift]
            if shift:
                mine = send(mine, pieces_of(inner, panel_size, shift), both)
            own_pieces.append(mine)
            guest_pieces.append(send(theirs, pieces_of(outward, panel_size, shift), both))

    split = (chunks - 1) * panel_size
    out = None
    for lo, hi, first, final in ((0, split, 0, chunks - 1), (split, chunks * panel_size, chunks - 1, chunks)):
        if lo == hi:
            continue
        pieces = own_pieces[lo:hi] + guest_pieces[lo:hi]
        before = [] if out is None else [out]
        out = pl.pallas_call(
            functools.partial(assemble_kernel, panel_size, starts[first:final], sizes[first:final], len(before)),
            out_shape=jax.ShapeDtypeStruct((rows // panel_size, width * panel_size), queries.dtype),
            in_specs=[in_smem] + [anywhere] * len(before) + [in_vmem] * len(pieces),
            out_specs=anywhere,
            scratch_shapes=[pltpu.SemaphoreType.DMA((panel_size, final - first))],
            input_output_aliases={1: 0} if before else {},
            compiler_params=pltpu.CompilerParams(vmem_limit_bytes=VMEM_GRANT),
        )(info, *before, *pieces)
    return out


def solution(mesh):
    seq_size, panel_size = mesh.shape["seq"], mesh.shape["panel"]
    relay = seq_size // CORES - 2 == 2
    if relay:
        body = functools.partial(relayed, seq_size=seq_size, panel_size=panel_size)
    else:
        body = functools.partial(gathered, seq_size=seq_size)
    return jax.shard_map(
        body,
        mesh=mesh,
        in_specs=(
            P(("groups", "seq"), "panel"),
            P(("groups", "seq"), "panel"),
            P(("groups", "seq"), "panel"),
            P("panel", None, None),
            P("panel", None),
        ),
        out_specs=P(("groups", "seq", "panel"), None),
        check_vma=False,
    )
```

```python
import functools

import jax
import jax.numpy as jnp
from jax import lax
from jax.experimental import pallas as pl
from jax.experimental.pallas import tpu as pltpu
from jax.sharding import PartitionSpec as P


HEAD_DIM = 128
BLOCK = 128
LOG2_E = 1.4426950408889634
DEAD = -1e30
CORES = 2
FIRST_SHARE = 8, 12
UNROLL = 4
EARLY_SLOTS = 0, 1, 2, 3, 4, 5
HOMES = 0, 4
VMEM_GRANT = 20 << 20


def tables(block_lists, block_counts, owner, seq_size):
    heads, tiles, listed = block_lists.shape
    per_index = tiles // seq_size
    lists = lax.dynamic_slice_in_dim(block_lists, owner * per_index, per_index, 1)
    counts = lax.dynamic_slice_in_dim(block_counts, owner * per_index, per_index, 1)
    slot_live = jnp.arange(listed, dtype=jnp.int32) < counts[:, :, None]
    ids = jnp.arange(tiles, dtype=jnp.int32)
    hits = (lists[:, :, :, None] == ids) & slot_live[:, :, :, None]
    keep = jnp.any(hits, axis=2).astype(jnp.int32).reshape(heads, per_index, seq_size, per_index)
    low, high = keep[..., 0], keep[..., 1]
    taken = jnp.max(high, axis=1)
    live = jnp.where(taken[:, None, :] == 1, high, low)
    other = jnp.where(taken[:, None, :] == 1, low, high)
    bits = jnp.array([2 << tile for tile in range(per_index)], jnp.int32)[None, :, None]
    code = taken + jnp.sum(live * bits, axis=1)
    code_other = (1 - taken) + jnp.sum(other * bits, axis=1)
    mine = jnp.arange(seq_size) == owner
    extra = jnp.sum(jnp.where(mine, code_other, 0), axis=1, keepdims=True)
    return jnp.concatenate([code, extra], axis=1)


def attend(query, codes, key_block, value_block):
    rows = query.shape[0]
    factor = HEAD_DIM ** (-0.5) * LOG2_E
    masked = []
    for j, code in enumerate(codes):
        scores = lax.dot_general(
            query, key_block(j, code & 1), (((1,), (1,)), ((), ())), preferred_element_type=jnp.float32
        )
        parts = []
        for tile in range(rows // BLOCK):
            bias = jnp.where((code >> (tile + 1)) & 1 == 1, 0.0, DEAD).astype(jnp.float32)
            parts.append(scores[tile * BLOCK : (tile + 1) * BLOCK] * factor + bias)
        masked.append(jnp.concatenate(parts, axis=0))
    top = jnp.max(functools.reduce(jnp.maximum, masked), axis=1, keepdims=True)
    total, mixed = None, None
    for j, code in enumerate(codes):
        weights = jnp.exp2(masked[j] - top)
        total = weights if total is None else total + weights
        product = jnp.dot(
            weights.astype(jnp.bfloat16), value_block(j, code & 1), preferred_element_type=jnp.float32
        )
        mixed = product if mixed is None else mixed + product
    return mixed / jnp.sum(total, axis=1, keepdims=True)


def gathered_kernel(seq_size, own_rows, info_ref, code_ref, query_ref, key_ref, value_ref, out_ref):
    head = pl.program_id(0)
    owner = info_ref[0]

    def block(ref):
        def read(j, which):
            index = owner if j == seq_size else j
            return ref[pl.ds(pl.multiple_of(index * own_rows + which * BLOCK, BLOCK), BLOCK), :]

        return read

    codes = [code_ref[head * (seq_size + 1) + j] for j in range(seq_size + 1)]
    out_ref[...] = attend(query_ref[...], codes, block(key_ref), block(value_ref)).astype(out_ref.dtype)


def gathered(queries, key_rows, value_rows, block_lists, block_counts, seq_size):
    rows, width = queries.shape
    heads = width // HEAD_DIM
    position = lax.axis_index("seq")
    keys = lax.all_gather(key_rows, "seq", axis=0, tiled=True)
    values = lax.all_gather(value_rows, "seq", axis=0, tiled=True)
    codes = tables(block_lists, block_counts, position, seq_size).reshape(-1)
    all_rows = keys.shape[0]
    out = pl.pallas_call(
        functools.partial(gathered_kernel, seq_size, rows),
        out_shape=jax.ShapeDtypeStruct((rows, width), queries.dtype),
        grid_spec=pltpu.PrefetchScalarGridSpec(
            num_scalar_prefetch=2,
            grid=(heads,),
            in_specs=[
                pl.BlockSpec((rows, HEAD_DIM), lambda h, *_: (0, h)),
                pl.BlockSpec((all_rows, HEAD_DIM), lambda h, *_: (0, h)),
                pl.BlockSpec((all_rows, HEAD_DIM), lambda h, *_: (0, h)),
            ],
            out_specs=pl.BlockSpec((rows, HEAD_DIM), lambda h, *_: (0, h)),
        ),
        name="attend_gathered",
    )(position.reshape(1), codes, queries, keys, values)
    return lax.all_to_all(out, "panel", split_axis=0, concat_axis=1, tiled=True)


def pieces_of(seq_pairs, panel_size, shift):
    return [
        (source * panel_size + panel, target * panel_size + (panel + shift) % panel_size)
        for source, target in seq_pairs
        for panel in range(panel_size)
    ]


def send(value, pairs, axes="seq"):
    return lax.ppermute(value, axes, pairs)


def pack_kernel(starts, sizes, key_ref, value_ref, *refs):
    outs, sems = refs[:-1], refs[-1]
    rows = key_ref.shape[0]
    copies = []
    for k, (start, size) in enumerate(zip(starts, sizes)):
        columns = pl.ds(start * HEAD_DIM, size * HEAD_DIM)
        for kind, ref in enumerate((key_ref, value_ref)):
            copies.append(
                pltpu.make_async_copy(ref.at[:, columns], outs[k].at[pl.ds(kind * rows, rows), :], sems.at[k, kind])
            )
            copies[-1].start()
    for copy in copies:
        copy.wait()


def masked_scores(query, codes, key_block):
    factor = HEAD_DIM ** (-0.5) * LOG2_E
    masked = []
    for j, code in codes:
        scores = lax.dot_general(
            key_block(j, code & 1), query, (((1,), (1,)), ((), ())), preferred_element_type=jnp.float32
        )
        tiles = query.shape[0] // BLOCK
        bias = [
            jnp.full((1, BLOCK), jnp.where((code >> (tile + 1)) & 1 == 1, 0.0, DEAD), jnp.float32)
            for tile in range(tiles)
        ]
        masked.append(scores * factor + jnp.concatenate(bias, axis=1))
    return masked


def weigh(masked, top, codes, value_block):
    total, mixed = None, None
    for scores, (j, code) in zip(masked, codes):
        weights = jnp.exp2(scores - top)
        total = weights if total is None else total + weights
        product = lax.dot_general(
            value_block(j, code & 1),
            weights.astype(jnp.bfloat16),
            (((0,), (0,)), ((), ())),
            preferred_element_type=jnp.float32,
        )
        mixed = product if mixed is None else mixed + product
    return jnp.sum(total, axis=0, keepdims=True), mixed


def highest(masked):
    return jnp.max(functools.reduce(jnp.maximum, masked), axis=0, keepdims=True)


def each_unit(count, unit):
    whole = count // UNROLL

    @pl.loop(0, whole)
    def _(group):
        for i in range(UNROLL):
            unit(group * UNROLL, i)

    for i in range(count - whole * UNROLL):
        unit(whole * UNROLL, i)


def columns_of(head):
    return pl.ds(pl.multiple_of(head * HEAD_DIM, HEAD_DIM), HEAD_DIM)


def block_reader(pick):
    def block(slot, which):
        ref, first, columns = pick(slot)
        return ref[pl.ds(pl.multiple_of(first + which * BLOCK, BLOCK), BLOCK), columns]

    return block


def early_kernel(seq_size, heads, starts, sizes, side, *refs):
    info_ref, code_ref, queries = refs[:3]
    whole = refs[3:11]
    near = refs[11 : 11 + 2 * (len(sizes) - 1)]
    sums = refs[11 + len(near) : 11 + len(near) + len(sizes)]
    stats = refs[11 + len(near) + len(sizes) :]
    rows = queries.shape[0]

    @pl.when(info_ref[0] == 1)
    def _():
        for k, (start, size) in enumerate(zip(starts, sizes)):
            slots = EARLY_SLOTS[: 4 if k == len(sizes) - 1 else 6]

            def unit(base, i):
                h = base + i
                columns = columns_of(h + start)
                first = (side * heads + h + start) * (seq_size + 1)
                codes = [(slot, code_ref[first + slot]) for slot in slots]
                if HOMES[side] in slots:
                    codes.append((HOMES[side], code_ref[first + seq_size]))

                def pick(kind, slot):
                    if slot < 4:
                        return whole[2 * slot + kind], 0, columns
                    return near[2 * k + slot - 4], kind * rows, columns_of(h)

                masked = masked_scores(queries[:, columns], codes, block_reader(functools.partial(pick, 0)))
                top = highest(masked)
                total, mixed = weigh(masked, top, codes, block_reader(functools.partial(pick, 1)))
                sums[k][h] = mixed
                stats[k][h, pl.ds(0, 1), :] = top
                stats[k][h, pl.ds(1, 1), :] = total

            each_unit(size, unit)


def late_kernel(seq_size, panel_size, heads, start, size, near, *refs):
    info_ref, code_ref = refs[:2]
    queries, sums, stats = refs[2:4], refs[4:6], refs[6:8]
    stacked = refs[8 : 8 + (4 if near else 2)]
    outs = refs[8 + len(stacked) : -1]
    held = refs[-1]
    panel = info_ref[1]
    rows = queries[0].shape[0]
    piece = rows // panel_size
    slots = range(seq_size - len(stacked), seq_size)

    def unit(base, i):
        h, side = base // 2 + i // 2, i % 2
        local = columns_of(h)
        first = (side * heads + h + start) * (seq_size + 1)
        codes = [(slot, code_ref[first + slot]) for slot in slots]
        if HOMES[side] in slots:
            codes.append((HOMES[side], code_ref[first + seq_size]))
        read = lambda kind: block_reader(lambda slot: (stacked[slot - slots[0]], kind * rows, local))
        masked = masked_scores(queries[side][:, columns_of(h + start)], codes, read(0))
        before = stats[side][h, pl.ds(0, 1), :]
        top = jnp.maximum(before, highest(masked))
        kept = jnp.exp2(before - top)
        total, mixed = weigh(masked, top, codes, read(1))
        total = total + kept * stats[side][h, pl.ds(1, 1), :]
        mixed = mixed + kept * sums[side][h]
        held[i] = (mixed / total).astype(held.dtype).T
        for shift in range(panel_size):
            first_row = pl.multiple_of(lax.rem(panel + shift, panel_size) * piece, piece)
            outs[side * panel_size + shift][:, local] = held[i, pl.ds(first_row, piece), :]

    @pl.when(info_ref[0] == 1)
    def _():
        each_unit(2 * size, unit)


def assemble_kernel(panel_size, starts, sizes, aliased, info_ref, *refs):
    out_ref, sems = refs[-2:]
    refs = refs[1:] if aliased else refs
    count = len(sizes)
    width = out_ref.shape[1] // panel_size
    panel = info_ref[1]
    inner = info_ref[0] == 1
    copies = []
    for shift in range(panel_size):
        source = lax.rem(panel + panel_size - shift, panel_size)
        for chunk, (start, size) in enumerate(zip(starts, sizes)):
            columns = pl.ds(pl.multiple_of(source * width + start * HEAD_DIM, HEAD_DIM), size * HEAD_DIM)
            own, guest = (
                pltpu.make_async_copy(
                    refs[(side * count + chunk) * panel_size + shift],
                    out_ref.at[:, columns],
                    sems.at[shift, chunk],
                )
                for side in range(2)
            )
            pl.when(inner)(own.start)
            pl.when(jnp.logical_not(inner))(guest.start)
            copies.append(own)
    for copy in copies:
        copy.wait()


def relayed(queries, key_rows, value_rows, block_lists, block_counts, seq_size, panel_size):
    rows, width = queries.shape
    heads = width // HEAD_DIM
    chips = seq_size // CORES
    position = lax.axis_index("seq")
    panel = lax.axis_index("panel")
    chip, core = position // CORES, position % CORES
    last = chips - 1
    cores = range(CORES)
    inward = [(source * CORES + c, target * CORES + c) for source, target in ((0, 1), (last, last - 1)) for c in cores]
    across = [(source * CORES + c, target * CORES + c) for source, target in ((1, 2), (2, 1)) for c in cores]
    partner = [(z * CORES + c, z * CORES + CORES - 1 - c) for z in (1, 2) for c in cores]
    inner = [(z * CORES + c, z * CORES + c) for z in (1, 2) for c in cores]
    outward = [(target, source) for source, target in inward]
    in_vmem, in_smem, anywhere = (pl.BlockSpec(memory_space=s) for s in (pltpu.VMEM, pltpu.SMEM, pl.ANY))

    front = max(1, heads * FIRST_SHARE[0] // FIRST_SHARE[1])
    sizes = [front, heads - front]
    starts = [0, front]
    chunks = len(sizes)

    middle = [send(x, across) for x in (key_rows, value_rows)]
    packed = pl.pallas_call(
        functools.partial(pack_kernel, starts, sizes),
        out_shape=[jax.ShapeDtypeStruct((2 * rows, size * HEAD_DIM), key_rows.dtype) for size in sizes],
        in_specs=[anywhere] * 2,
        out_specs=[in_vmem] * chunks,
        scratch_shapes=[pltpu.SemaphoreType.DMA((chunks, 2))],
        compiler_params=pltpu.CompilerParams(vmem_limit_bytes=VMEM_GRANT),
        name="pack",
    )(key_rows, value_rows)
    beside = [send(x, partner) for x in (key_rows, value_rows)]
    ends = [send(x, inward) for x in packed]
    guest_query = send(queries, inward)
    middle_beside = [send(x, partner) for x in middle]

    is_inner = (chip >= 1) & (chip < last)
    end = jnp.where(chip * 2 < chips, 0, last)
    guest = end * CORES + core
    order = jnp.stack(
        [
            z * CORES + c
            for z in (chip, last - chip, end, last - end)
            for c in (core, CORES - 1 - core)
        ]
    )
    pick = (order[:, None] == jnp.arange(seq_size)).astype(jnp.int32)

    def arranged(owner):
        codes = tables(block_lists, block_counts, owner, seq_size)
        return jnp.concatenate([jnp.sum(codes[:, None, :seq_size] * pick, axis=2), codes[:, seq_size:]], axis=1)

    codes = jnp.stack([arranged(position), arranged(guest)]).reshape(-1)
    info = jnp.stack([is_inner.astype(jnp.int32), panel])

    params = pltpu.CompilerParams(vmem_limit_bytes=VMEM_GRANT)
    cost = lambda count, blocks: pl.CostEstimate(
        flops=count * 4 * rows * blocks * BLOCK * HEAD_DIM,
        bytes_accessed=count * blocks * 4 * BLOCK * HEAD_DIM,
        transcendentals=count * rows * blocks * BLOCK,
    )
    ends_beside = [send(x, partner) for x in ends]
    near = [x for pair in zip(ends, ends_beside) for x in pair]
    early = []
    for side, side_queries in enumerate((queries, guest_query)):
        early.append(
            pl.pallas_call(
                functools.partial(early_kernel, seq_size, heads, starts, sizes, side),
                out_shape=[jax.ShapeDtypeStruct((size, HEAD_DIM, rows), jnp.float32) for size in sizes]
                + [jax.ShapeDtypeStruct((size, 8, rows), jnp.float32) for size in sizes],
                in_specs=[in_smem] * 2 + [in_vmem] * (9 + 2 * (chunks - 1)),
                out_specs=[in_vmem] * (2 * chunks),
                compiler_params=params,
                cost_estimate=cost(heads, 6),
            )(info, codes, side_queries, key_rows, value_rows, *beside, *middle, *middle_beside, *near[:-2])
        )

    own_pieces, guest_pieces = [], []
    for k, (start, size) in enumerate(zip(starts, sizes)):
        far = send(ends[k], across)
        stacked = [far, send(far, partner)]
        if k == chunks - 1:
            stacked = near[-2:] + stacked
        outs = pl.pallas_call(
            functools.partial(late_kernel, seq_size, panel_size, heads, start, size, len(stacked) == 4),
            out_shape=[jax.ShapeDtypeStruct((rows // panel_size, size * HEAD_DIM), queries.dtype)] * (2 * panel_size),
            in_specs=[in_smem] * 2 + [in_vmem] * (6 + len(stacked)),
            out_specs=[in_vmem] * (2 * panel_size),
            scratch_shapes=[pltpu.VMEM((UNROLL, rows, HEAD_DIM), queries.dtype)],
            compiler_params=params,
            cost_estimate=cost(2 * size, len(stacked)),
        )(
            *(info, codes, queries, guest_query),
            *(early[side][k] for side in range(2)),
            *(early[side][chunks + k] for side in range(2)),
            *stacked,
        )
        both = ("seq", "panel")
        for shift in range(panel_size):
            mine, theirs = outs[shift], outs[panel_size + shift]
            if shift:
                mine = send(mine, pieces_of(inner, panel_size, shift), both)
            own_pieces.append(mine)
            guest_pieces.append(send(theirs, pieces_of(outward, panel_size, shift), both))

    split = (chunks - 1) * panel_size
    out = None
    for lo, hi, first, final in ((0, split, 0, chunks - 1), (split, chunks * panel_size, chunks - 1, chunks)):
        if lo == hi:
            continue
        pieces = own_pieces[lo:hi] + guest_pieces[lo:hi]
        before = [] if out is None else [out]
        out = pl.pallas_call(
            functools.partial(assemble_kernel, panel_size, starts[first:final], sizes[first:final], len(before)),
            out_shape=jax.ShapeDtypeStruct((rows // panel_size, width * panel_size), queries.dtype),
            in_specs=[in_smem] + [anywhere] * len(before) + [in_vmem] * len(pieces),
            out_specs=anywhere,
            scratch_shapes=[pltpu.SemaphoreType.DMA((panel_size, final - first))],
            input_output_aliases={1: 0} if before else {},
            compiler_params=pltpu.CompilerParams(vmem_limit_bytes=VMEM_GRANT),
        )(info, *before, *pieces)
    return out


def solution(mesh):
    seq_size, panel_size = mesh.shape["seq"], mesh.shape["panel"]
    relay = seq_size // CORES - 2 == 2
    if relay:
        body = functools.partial(relayed, seq_size=seq_size, panel_size=panel_size)
    else:
        body = functools.partial(gathered, seq_size=seq_size)
    return jax.shard_map(
        body,
        mesh=mesh,
        in_specs=(
            P(("groups", "seq"), "panel"),
            P(("groups", "seq"), "panel"),
            P(("groups", "seq"), "panel"),
            P("panel", None, None),
            P("panel", None),
        ),
        out_specs=P(("groups", "seq", "panel"), None),
        check_vma=False,
    )
```

```python
import functools

import jax
import jax.numpy as jnp
from jax import lax
from jax.experimental import pallas as pl
from jax.experimental.pallas import tpu as pltpu
from jax.sharding import PartitionSpec as P


HEAD_DIM = 128
BLOCK = 128
LOG2_E = 1.4426950408889634
DEAD = -1e30
CORES = 2
FIRST_SHARE = 8, 12
UNROLL = 4
EARLY_SLOTS = 0, 1, 2, 3, 4, 5
HOMES = 0, 4
EARLY_CALLS = (0, (0, 1)), (1, (0,)), (1, (1,))
VMEM_GRANT = 20 << 20


def tables(block_lists, block_counts, owner, seq_size):
    heads, tiles, listed = block_lists.shape
    per_index = tiles // seq_size
    lists = lax.dynamic_slice_in_dim(block_lists, owner * per_index, per_index, 1)
    counts = lax.dynamic_slice_in_dim(block_counts, owner * per_index, per_index, 1)
    slot_live = jnp.arange(listed, dtype=jnp.int32) < counts[:, :, None]
    ids = jnp.arange(tiles, dtype=jnp.int32)
    hits = (lists[:, :, :, None] == ids) & slot_live[:, :, :, None]
    keep = jnp.any(hits, axis=2).astype(jnp.int32).reshape(heads, per_index, seq_size, per_index)
    low, high = keep[..., 0], keep[..., 1]
    taken = jnp.max(high, axis=1)
    live = jnp.where(taken[:, None, :] == 1, high, low)
    other = jnp.where(taken[:, None, :] == 1, low, high)
    bits = jnp.array([2 << tile for tile in range(per_index)], jnp.int32)[None, :, None]
    code = taken + jnp.sum(live * bits, axis=1)
    code_other = (1 - taken) + jnp.sum(other * bits, axis=1)
    mine = jnp.arange(seq_size) == owner
    extra = jnp.sum(jnp.where(mine, code_other, 0), axis=1, keepdims=True)
    return jnp.concatenate([code, extra], axis=1)


def attend(query, codes, key_block, value_block):
    rows = query.shape[0]
    factor = HEAD_DIM ** (-0.5) * LOG2_E
    masked = []
    for j, code in enumerate(codes):
        scores = lax.dot_general(
            query, key_block(j, code & 1), (((1,), (1,)), ((), ())), preferred_element_type=jnp.float32
        )
        parts = []
        for tile in range(rows // BLOCK):
            bias = jnp.where((code >> (tile + 1)) & 1 == 1, 0.0, DEAD).astype(jnp.float32)
            parts.append(scores[tile * BLOCK : (tile + 1) * BLOCK] * factor + bias)
        masked.append(jnp.concatenate(parts, axis=0))
    top = jnp.max(functools.reduce(jnp.maximum, masked), axis=1, keepdims=True)
    total, mixed = None, None
    for j, code in enumerate(codes):
        weights = jnp.exp2(masked[j] - top)
        total = weights if total is None else total + weights
        product = jnp.dot(
            weights.astype(jnp.bfloat16), value_block(j, code & 1), preferred_element_type=jnp.float32
        )
        mixed = product if mixed is None else mixed + product
    return mixed / jnp.sum(total, axis=1, keepdims=True)


def gathered_kernel(seq_size, own_rows, info_ref, code_ref, query_ref, key_ref, value_ref, out_ref):
    head = pl.program_id(0)
    owner = info_ref[0]

    def block(ref):
        def read(j, which):
            index = owner if j == seq_size else j
            return ref[pl.ds(pl.multiple_of(index * own_rows + which * BLOCK, BLOCK), BLOCK), :]

        return read

    codes = [code_ref[head * (seq_size + 1) + j] for j in range(seq_size + 1)]
    out_ref[...] = attend(query_ref[...], codes, block(key_ref), block(value_ref)).astype(out_ref.dtype)


def gathered(queries, key_rows, value_rows, block_lists, block_counts, seq_size):
    rows, width = queries.shape
    heads = width // HEAD_DIM
    position = lax.axis_index("seq")
    keys = lax.all_gather(key_rows, "seq", axis=0, tiled=True)
    values = lax.all_gather(value_rows, "seq", axis=0, tiled=True)
    codes = tables(block_lists, block_counts, position, seq_size).reshape(-1)
    all_rows = keys.shape[0]
    out = pl.pallas_call(
        functools.partial(gathered_kernel, seq_size, rows),
        out_shape=jax.ShapeDtypeStruct((rows, width), queries.dtype),
        grid_spec=pltpu.PrefetchScalarGridSpec(
            num_scalar_prefetch=2,
            grid=(heads,),
            in_specs=[
                pl.BlockSpec((rows, HEAD_DIM), lambda h, *_: (0, h)),
                pl.BlockSpec((all_rows, HEAD_DIM), lambda h, *_: (0, h)),
                pl.BlockSpec((all_rows, HEAD_DIM), lambda h, *_: (0, h)),
            ],
            out_specs=pl.BlockSpec((rows, HEAD_DIM), lambda h, *_: (0, h)),
        ),
        name="attend_gathered",
    )(position.reshape(1), codes, queries, keys, values)
    return lax.all_to_all(out, "panel", split_axis=0, concat_axis=1, tiled=True)


def pieces_of(seq_pairs, panel_size, shift):
    return [
        (source * panel_size + panel, target * panel_size + (panel + shift) % panel_size)
        for source, target in seq_pairs
        for panel in range(panel_size)
    ]


def send(value, pairs, axes="seq"):
    return lax.ppermute(value, axes, pairs)


def pack_kernel(starts, sizes, key_ref, value_ref, query_ref, *refs):
    outs, query_outs, sems = refs[: len(sizes)], refs[len(sizes) : -1], refs[-1]
    rows = key_ref.shape[0]
    copies = []
    for k, (start, size) in enumerate(zip(starts, sizes)):
        columns = pl.ds(start * HEAD_DIM, size * HEAD_DIM)
        targets = outs[k].at[pl.ds(0, rows), :], outs[k].at[pl.ds(rows, rows), :], query_outs[k]
        for kind, ref in enumerate((key_ref, value_ref, query_ref)):
            copies.append(pltpu.make_async_copy(ref.at[:, columns], targets[kind], sems.at[k, kind]))
            copies[-1].start()
    for copy in copies:
        copy.wait()


def masked_scores(query, codes, key_block):
    factor = HEAD_DIM ** (-0.5) * LOG2_E
    masked = []
    for j, code in codes:
        scores = lax.dot_general(
            key_block(j, code & 1), query, (((1,), (1,)), ((), ())), preferred_element_type=jnp.float32
        )
        tiles = query.shape[0] // BLOCK
        bias = [
            jnp.full((1, BLOCK), jnp.where((code >> (tile + 1)) & 1 == 1, 0.0, DEAD), jnp.float32)
            for tile in range(tiles)
        ]
        masked.append(scores * factor + jnp.concatenate(bias, axis=1))
    return masked


def weigh(masked, top, codes, value_block):
    total, mixed = None, None
    for scores, (j, code) in zip(masked, codes):
        weights = jnp.exp2(scores - top)
        total = weights if total is None else total + weights
        product = lax.dot_general(
            value_block(j, code & 1),
            weights.astype(jnp.bfloat16),
            (((0,), (0,)), ((), ())),
            preferred_element_type=jnp.float32,
        )
        mixed = product if mixed is None else mixed + product
    return jnp.sum(total, axis=0, keepdims=True), mixed


def highest(masked):
    return jnp.max(functools.reduce(jnp.maximum, masked), axis=0, keepdims=True)


def each_unit(count, unit):
    whole = count // UNROLL

    @pl.loop(0, whole)
    def _(group):
        for i in range(UNROLL):
            unit(group * UNROLL, i)

    for i in range(count - whole * UNROLL):
        unit(whole * UNROLL, i)


def columns_of(head):
    return pl.ds(pl.multiple_of(head * HEAD_DIM, HEAD_DIM), HEAD_DIM)


def block_reader(pick):
    def block(slot, which):
        ref, first, columns = pick(slot)
        return ref[pl.ds(pl.multiple_of(first + which * BLOCK, BLOCK), BLOCK), columns]

    return block


def early_kernel(seq_size, heads, starts, sizes, chunks, side, *refs):
    info_ref, code_ref = refs[:2]
    count = len(chunks)
    near_count = sum(k < len(sizes) - 1 for k in chunks)
    whole = refs[2:10]
    refs = refs[10:]
    queries, refs = refs[:count], refs[count:]
    near, refs = refs[: 2 * near_count], refs[2 * near_count :]
    sums, stats = refs[:count], refs[count : 2 * count]
    held, sems = refs[2 * count :]
    groups = [
        (n, k, low, min(low + UNROLL, sizes[k])) for n, k in enumerate(chunks) for low in range(0, sizes[k], UNROLL)
    ]

    def loads(g):
        _, k, low, high = groups[g]
        width = (high - low) * HEAD_DIM
        source = pl.ds((starts[k] + low) * HEAD_DIM, width)
        return [
            pltpu.make_async_copy(
                ref.at[:, source], held.at[g % 2, index, :, pl.ds(0, width)], sems.at[g % 2, index]
            )
            for index, ref in enumerate(whole)
        ]

    @pl.when(info_ref[0] == 1)
    def _():
        for copy in loads(0):
            copy.start()
        for g, (n, k, low, high) in enumerate(groups):
            if g + 1 < len(groups):
                for copy in loads(g + 1):
                    copy.start()
            for copy in loads(g):
                copy.wait()
            slots = EARLY_SLOTS[: 4 if k == len(sizes) - 1 else 6]
            for h in range(low, high):
                first = (side * heads + h + starts[k]) * (seq_size + 1)
                codes = [(slot, code_ref[first + slot]) for slot in slots]
                if HOMES[side] in slots:
                    codes.append((HOMES[side], code_ref[first + seq_size]))
                local = pl.ds(h * HEAD_DIM, HEAD_DIM)

                def pick(kind, slot):
                    if slot < 4:
                        return held.at[g % 2, 2 * slot + kind], 0, pl.ds((h - low) * HEAD_DIM, HEAD_DIM)
                    return near[2 * n + slot - 4], kind * held.shape[2], local

                masked = masked_scores(queries[n][:, local], codes, block_reader(functools.partial(pick, 0)))
                top = highest(masked)
                total, mixed = weigh(masked, top, codes, block_reader(functools.partial(pick, 1)))
                sums[n][h] = mixed
                stats[n][h, pl.ds(0, 1), :] = top
                stats[n][h, pl.ds(1, 1), :] = total


def late_kernel(seq_size, panel_size, heads, start, size, near, *refs):
    info_ref, code_ref = refs[:2]
    queries, sums, stats = refs[2:4], refs[4:6], refs[6:8]
    stacked = refs[8 : 8 + (4 if near else 2)]
    outs = refs[8 + len(stacked) : -1]
    held = refs[-1]
    panel = info_ref[1]
    rows = queries[0].shape[0]
    piece = rows // panel_size
    slots = range(seq_size - len(stacked), seq_size)

    def unit(base, i):
        h, side = base // 2 + i // 2, i % 2
        local = columns_of(h)
        first = (side * heads + h + start) * (seq_size + 1)
        codes = [(slot, code_ref[first + slot]) for slot in slots]
        if HOMES[side] in slots:
            codes.append((HOMES[side], code_ref[first + seq_size]))
        read = lambda kind: block_reader(lambda slot: (stacked[slot - slots[0]], kind * rows, local))
        masked = masked_scores(queries[side][:, local], codes, read(0))
        before = stats[side][h, pl.ds(0, 1), :]
        top = jnp.maximum(before, highest(masked))
        kept = jnp.exp2(before - top)
        total, mixed = weigh(masked, top, codes, read(1))
        total = total + kept * stats[side][h, pl.ds(1, 1), :]
        mixed = mixed + kept * sums[side][h]
        held[i] = (mixed / total).astype(held.dtype).T
        for shift in range(panel_size):
            first_row = pl.multiple_of(lax.rem(panel + shift, panel_size) * piece, piece)
            outs[side * panel_size + shift][:, local] = held[i, pl.ds(first_row, piece), :]

    @pl.when(info_ref[0] == 1)
    def _():
        each_unit(2 * size, unit)


def assemble_kernel(panel_size, starts, sizes, aliased, info_ref, *refs):
    out_ref, sems = refs[-2:]
    refs = refs[1:] if aliased else refs
    count = len(sizes)
    width = out_ref.shape[1] // panel_size
    panel = info_ref[1]
    inner = info_ref[0] == 1
    copies = []
    for shift in range(panel_size):
        source = lax.rem(panel + panel_size - shift, panel_size)
        for chunk, (start, size) in enumerate(zip(starts, sizes)):
            columns = pl.ds(pl.multiple_of(source * width + start * HEAD_DIM, HEAD_DIM), size * HEAD_DIM)
            own, guest = (
                pltpu.make_async_copy(
                    refs[(side * count + chunk) * panel_size + shift],
                    out_ref.at[:, columns],
                    sems.at[shift, chunk],
                )
                for side in range(2)
            )
            pl.when(inner)(own.start)
            pl.when(jnp.logical_not(inner))(guest.start)
            copies.append(own)
    for copy in copies:
        copy.wait()


def relayed(queries, key_rows, value_rows, block_lists, block_counts, seq_size, panel_size):
    rows, width = queries.shape
    heads = width // HEAD_DIM
    chips = seq_size // CORES
    position = lax.axis_index("seq")
    panel = lax.axis_index("panel")
    chip, core = position // CORES, position % CORES
    last = chips - 1
    cores = range(CORES)
    inward = [(source * CORES + c, target * CORES + c) for source, target in ((0, 1), (last, last - 1)) for c in cores]
    across = [(source * CORES + c, target * CORES + c) for source, target in ((1, 2), (2, 1)) for c in cores]
    partner = [(z * CORES + c, z * CORES + CORES - 1 - c) for z in (1, 2) for c in cores]
    inner = [(z * CORES + c, z * CORES + c) for z in (1, 2) for c in cores]
    outward = [(target, source) for source, target in inward]
    in_vmem, in_smem, in_hbm, anywhere = (
        pl.BlockSpec(memory_space=space) for space in (pltpu.VMEM, pltpu.SMEM, pltpu.MemorySpace.HBM, pl.ANY)
    )

    front = max(1, heads * FIRST_SHARE[0] // FIRST_SHARE[1])
    sizes = [front, heads - front]
    starts = [0, front]
    chunks = len(sizes)

    middle = [send(x, across) for x in (key_rows, value_rows)]
    packed = pl.pallas_call(
        functools.partial(pack_kernel, starts, sizes),
        out_shape=[jax.ShapeDtypeStruct((2 * rows, size * HEAD_DIM), key_rows.dtype) for size in sizes]
        + [jax.ShapeDtypeStruct((rows, size * HEAD_DIM), queries.dtype) for size in sizes],
        in_specs=[in_hbm] * 3,
        out_specs=[in_vmem] * (2 * chunks),
        scratch_shapes=[pltpu.SemaphoreType.DMA((chunks, 3))],
        compiler_params=pltpu.CompilerParams(vmem_limit_bytes=VMEM_GRANT),
        name="pack",
    )(key_rows, value_rows, queries)
    packed, own_queries = packed[:chunks], packed[chunks:]
    beside = [send(x, partner) for x in (key_rows, value_rows)]
    ends = [send(x, inward) for x in packed]
    guest_queries = [send(x, inward) for x in own_queries]
    middle_beside = [send(x, partner) for x in middle]

    is_inner = (chip >= 1) & (chip < last)
    end = jnp.where(chip * 2 < chips, 0, last)
    guest = end * CORES + core
    order = jnp.stack(
        [
            z * CORES + c
            for z in (chip, last - chip, end, last - end)
            for c in (core, CORES - 1 - core)
        ]
    )
    pick = (order[:, None] == jnp.arange(seq_size)).astype(jnp.int32)

    def arranged(owner):
        codes = tables(block_lists, block_counts, owner, seq_size)
        return jnp.concatenate([jnp.sum(codes[:, None, :seq_size] * pick, axis=2), codes[:, seq_size:]], axis=1)

    codes = jnp.stack([arranged(position), arranged(guest)]).reshape(-1)
    info = jnp.stack([is_inner.astype(jnp.int32), panel])

    params = pltpu.CompilerParams(vmem_limit_bytes=VMEM_GRANT)
    cost = lambda count, blocks: pl.CostEstimate(
        flops=count * 4 * rows * blocks * BLOCK * HEAD_DIM,
        bytes_accessed=count * blocks * 4 * BLOCK * HEAD_DIM,
        transcendentals=count * rows * blocks * BLOCK,
    )
    ends_beside = [send(x, partner) for x in ends]
    near = [x for pair in zip(ends, ends_beside) for x in pair]
    sums, stats = {}, {}
    for side, some in EARLY_CALLS:
        side_queries = (own_queries, guest_queries)[side]
        near_end = [x for k in some if k < chunks - 1 for x in near[2 * k : 2 * k + 2]]
        results = pl.pallas_call(
            functools.partial(early_kernel, seq_size, heads, starts, sizes, some, side),
            out_shape=[jax.ShapeDtypeStruct((sizes[k], HEAD_DIM, rows), jnp.float32) for k in some]
            + [jax.ShapeDtypeStruct((sizes[k], 8, rows), jnp.float32) for k in some],
            in_specs=[in_smem] * 2 + [in_hbm] * 8 + [in_vmem] * (len(some) + len(near_end)),
            out_specs=[in_vmem] * (2 * len(some)),
            scratch_shapes=[
                pltpu.VMEM((2, 8, rows, UNROLL * HEAD_DIM), key_rows.dtype),
                pltpu.SemaphoreType.DMA((2, 8)),
            ],
            compiler_params=params,
            cost_estimate=cost(sum(sizes[k] for k in some), 6),
        )(
            *(info, codes, key_rows, value_rows, *beside, *middle, *middle_beside),
            *(side_queries[k] for k in some),
            *near_end,
        )
        for n, k in enumerate(some):
            sums[side, k], stats[side, k] = results[n], results[len(some) + n]

    own_pieces, guest_pieces = [], []
    for k, (start, size) in enumerate(zip(starts, sizes)):
        far = send(ends[k], across)
        stacked = [far, send(far, partner)]
        if k == chunks - 1:
            stacked = near[-2:] + stacked
        outs = pl.pallas_call(
            functools.partial(late_kernel, seq_size, panel_size, heads, start, size, len(stacked) == 4),
            out_shape=[jax.ShapeDtypeStruct((rows // panel_size, size * HEAD_DIM), queries.dtype)] * (2 * panel_size),
            in_specs=[in_smem] * 2 + [in_vmem] * (6 + len(stacked)),
            out_specs=[in_vmem] * (2 * panel_size),
            scratch_shapes=[pltpu.VMEM((UNROLL, rows, HEAD_DIM), queries.dtype)],
            compiler_params=params,
            cost_estimate=cost(2 * size, len(stacked)),
        )(
            *(info, codes, own_queries[k], guest_queries[k]),
            *(sums[side, k] for side in range(2)),
            *(stats[side, k] for side in range(2)),
            *stacked,
        )
        both = ("seq", "panel")
        for shift in range(panel_size):
            mine, theirs = outs[shift], outs[panel_size + shift]
            if shift:
                mine = send(mine, pieces_of(inner, panel_size, shift), both)
            own_pieces.append(mine)
            guest_pieces.append(send(theirs, pieces_of(outward, panel_size, shift), both))

    split = (chunks - 1) * panel_size
    out = None
    for lo, hi, first, final in ((0, split, 0, chunks - 1), (split, chunks * panel_size, chunks - 1, chunks)):
        if lo == hi:
            continue
        pieces = own_pieces[lo:hi] + guest_pieces[lo:hi]
        before = [] if out is None else [out]
        out = pl.pallas_call(
            functools.partial(assemble_kernel, panel_size, starts[first:final], sizes[first:final], len(before)),
            out_shape=jax.ShapeDtypeStruct((rows // panel_size, width * panel_size), queries.dtype),
            in_specs=[in_smem] + [anywhere] * len(before) + [in_vmem] * len(pieces),
            out_specs=anywhere,
            scratch_shapes=[pltpu.SemaphoreType.DMA((panel_size, final - first))],
            input_output_aliases={1: 0} if before else {},
            compiler_params=pltpu.CompilerParams(vmem_limit_bytes=VMEM_GRANT),
        )(info, *before, *pieces)
    return out


def solution(mesh):
    seq_size, panel_size = mesh.shape["seq"], mesh.shape["panel"]
    relay = seq_size // CORES - 2 == 2
    if relay:
        body = functools.partial(relayed, seq_size=seq_size, panel_size=panel_size)
    else:
        body = functools.partial(gathered, seq_size=seq_size)
    return jax.shard_map(
        body,
        mesh=mesh,
        in_specs=(
            P(("groups", "seq"), "panel"),
            P(("groups", "seq"), "panel"),
            P(("groups", "seq"), "panel"),
            P("panel", None, None),
            P("panel", None),
        ),
        out_specs=P(("groups", "seq", "panel"), None),
        check_vma=False,
    )
```

```python
import functools

import jax
import jax.numpy as jnp
from jax import lax
from jax.experimental import pallas as pl
from jax.experimental.pallas import tpu as pltpu
from jax.sharding import PartitionSpec as P


HEAD_DIM = 128
BLOCK = 128
LOG2_E = 1.4426950408889634
DEAD = -1e30
CORES = 2
FIRST_SHARE = 7, 12
UNROLL = 5
VMEM_GRANT = 14 << 20
HOMES = 0, 4
STAGES = (
    ("early_0", ((0, 0, (0, 1), False), (0, 1, (0, 1), False))),
    ("early_1", ((0, 0, (2, 3, 4, 5), True), (0, 1, (2, 3), True))),
    ("early_2", ((1, 0, (0, 1, 2, 3, 4, 5), False),)),
    ("early_3", ((1, 1, (0, 1, 2, 3, 4, 5), False), (0, 1, (4, 5), True))),
    ("late_0", ((0, 0, (6, 7), True), (1, 0, (6, 7), True))),
    ("late_1", ((0, 1, (6, 7), True), (1, 1, (6, 7), True))),
)


def tables(block_lists, block_counts, owner, seq_size):
    heads, tiles, listed = block_lists.shape
    per_index = tiles // seq_size
    lists = lax.dynamic_slice_in_dim(block_lists, owner * per_index, per_index, 1)
    counts = lax.dynamic_slice_in_dim(block_counts, owner * per_index, per_index, 1)
    slot_live = jnp.arange(listed, dtype=jnp.int32) < counts[:, :, None]
    ids = jnp.arange(tiles, dtype=jnp.int32)
    hits = (lists[:, :, :, None] == ids) & slot_live[:, :, :, None]
    keep = jnp.any(hits, axis=2).astype(jnp.int32).reshape(heads, per_index, seq_size, per_index)
    low, high = keep[..., 0], keep[..., 1]
    taken = jnp.max(high, axis=1)
    live = jnp.where(taken[:, None, :] == 1, high, low)
    other = jnp.where(taken[:, None, :] == 1, low, high)
    bits = jnp.array([2 << tile for tile in range(per_index)], jnp.int32)[None, :, None]
    code = taken + jnp.sum(live * bits, axis=1)
    code_other = (1 - taken) + jnp.sum(other * bits, axis=1)
    mine = jnp.arange(seq_size) == owner
    extra = jnp.sum(jnp.where(mine, code_other, 0), axis=1, keepdims=True)
    return jnp.concatenate([code, extra], axis=1)


def attend(query, codes, key_block, value_block):
    rows = query.shape[0]
    factor = HEAD_DIM ** (-0.5) * LOG2_E
    masked = []
    for j, code in enumerate(codes):
        scores = lax.dot_general(
            query, key_block(j, code & 1), (((1,), (1,)), ((), ())), preferred_element_type=jnp.float32
        )
        parts = []
        for tile in range(rows // BLOCK):
            bias = jnp.where((code >> (tile + 1)) & 1 == 1, 0.0, DEAD).astype(jnp.float32)
            parts.append(scores[tile * BLOCK : (tile + 1) * BLOCK] * factor + bias)
        masked.append(jnp.concatenate(parts, axis=0))
    top = jnp.max(functools.reduce(jnp.maximum, masked), axis=1, keepdims=True)
    total, mixed = None, None
    for j, code in enumerate(codes):
        weights = jnp.exp2(masked[j] - top)
        total = weights if total is None else total + weights
        product = jnp.dot(
            weights.astype(jnp.bfloat16), value_block(j, code & 1), preferred_element_type=jnp.float32
        )
        mixed = product if mixed is None else mixed + product
    return mixed / jnp.sum(total, axis=1, keepdims=True)


def gathered_kernel(seq_size, own_rows, info_ref, code_ref, query_ref, key_ref, value_ref, out_ref):
    head = pl.program_id(0)
    owner = info_ref[0]

    def block(ref):
        def read(j, which):
            index = owner if j == seq_size else j
            return ref[pl.ds(pl.multiple_of(index * own_rows + which * BLOCK, BLOCK), BLOCK), :]

        return read

    codes = [code_ref[head * (seq_size + 1) + j] for j in range(seq_size + 1)]
    out_ref[...] = attend(query_ref[...], codes, block(key_ref), block(value_ref)).astype(out_ref.dtype)


def gathered(queries, key_rows, value_rows, block_lists, block_counts, seq_size):
    rows, width = queries.shape
    heads = width // HEAD_DIM
    position = lax.axis_index("seq")
    keys = lax.all_gather(key_rows, "seq", axis=0, tiled=True)
    values = lax.all_gather(value_rows, "seq", axis=0, tiled=True)
    codes = tables(block_lists, block_counts, position, seq_size).reshape(-1)
    all_rows = keys.shape[0]
    out = pl.pallas_call(
        functools.partial(gathered_kernel, seq_size, rows),
        out_shape=jax.ShapeDtypeStruct((rows, width), queries.dtype),
        grid_spec=pltpu.PrefetchScalarGridSpec(
            num_scalar_prefetch=2,
            grid=(heads,),
            in_specs=[
                pl.BlockSpec((rows, HEAD_DIM), lambda h, *_: (0, h)),
                pl.BlockSpec((all_rows, HEAD_DIM), lambda h, *_: (0, h)),
                pl.BlockSpec((all_rows, HEAD_DIM), lambda h, *_: (0, h)),
            ],
            out_specs=pl.BlockSpec((rows, HEAD_DIM), lambda h, *_: (0, h)),
        ),
        name="attend_gathered",
    )(position.reshape(1), codes, queries, keys, values)
    return lax.all_to_all(out, "panel", split_axis=0, concat_axis=1, tiled=True)


def pieces_of(seq_pairs, panel_size, shift):
    return [
        (source * panel_size + panel, target * panel_size + (panel + shift) % panel_size)
        for source, target in seq_pairs
        for panel in range(panel_size)
    ]


def send(value, pairs, axes="seq"):
    return lax.ppermute(value, axes, pairs)


def pack_kernel(starts, sizes, chunk, *refs):
    sources, out, sems = refs[:-2], refs[-2], refs[-1]
    rows = sources[0].shape[0]
    columns = pl.ds(starts[chunk] * HEAD_DIM, sizes[chunk] * HEAD_DIM)
    copies = [
        pltpu.make_async_copy(ref.at[:, columns], out.at[pl.ds(kind * rows, rows), :], sems.at[kind])
        for kind, ref in enumerate(sources)
    ]
    for copy in copies:
        copy.start()
    for copy in copies:
        copy.wait()


def masked_scores(query, codes, key_block):
    factor = HEAD_DIM ** (-0.5) * LOG2_E
    masked = []
    for j, code in codes:
        scores = lax.dot_general(
            key_block(j, code & 1), query, (((1,), (1,)), ((), ())), preferred_element_type=jnp.float32
        )
        tiles = query.shape[0] // BLOCK
        bias = [
            jnp.full((1, BLOCK), jnp.where((code >> (tile + 1)) & 1 == 1, 0.0, DEAD), jnp.float32)
            for tile in range(tiles)
        ]
        masked.append(scores * factor + jnp.concatenate(bias, axis=1))
    return masked


def weigh(masked, top, codes, value_block):
    total, mixed = None, None
    for scores, (j, code) in zip(masked, codes):
        weights = jnp.exp2(scores - top)
        total = weights if total is None else total + weights
        product = lax.dot_general(
            value_block(j, code & 1),
            weights.astype(jnp.bfloat16),
            (((0,), (0,)), ((), ())),
            preferred_element_type=jnp.float32,
        )
        mixed = product if mixed is None else mixed + product
    return jnp.sum(total, axis=0, keepdims=True), mixed


def highest(masked):
    return jnp.max(functools.reduce(jnp.maximum, masked), axis=0, keepdims=True)


def each_unit(count, unit):
    groups = -(-count // UNROLL)
    size = -(-count // groups)
    whole = count // size

    @pl.loop(0, whole)
    def _(group):
        for i in range(size):
            unit(group * size, i)

    for i in range(count - whole * size):
        unit(whole * size, i)


def columns_of(head):
    return pl.ds(pl.multiple_of(head * HEAD_DIM, HEAD_DIM), HEAD_DIM)


def block_reader(pick):
    def block(slot, which):
        ref, first, columns = pick(slot)
        return ref[pl.ds(pl.multiple_of(first + which * BLOCK, BLOCK), BLOCK), columns]

    return block


def stage_kernel(seq_size, panel_size, heads, starts, sizes, jobs, inputs, final, *refs):
    info_ref, code_ref = refs[:2]
    have = dict(zip(inputs, refs[2:]))
    results = refs[2 + len(inputs) :]
    panel = info_ref[1]

    def job(n, side, k, slots, carry):
        queries = have["query", side, k]
        rows = queries.shape[0]
        piece = rows // panel_size

        def unit(base, i):
            h = base + i
            local = columns_of(h)
            first = (side * heads + h + starts[k]) * (seq_size + 1)
            codes = [(slot, code_ref[first + slot]) for slot in slots]
            if HOMES[side] in slots:
                codes.append((HOMES[side], code_ref[first + seq_size]))

            def pick(kind, slot):
                if ("chunk", slot, k) in have:
                    return have["chunk", slot, k], kind * rows, local
                return have["whole", slot, kind], 0, columns_of(h + starts[k])

            masked = masked_scores(queries[:, local], codes, block_reader(functools.partial(pick, 0)))
            top = highest(masked)
            if carry:
                stat = have["stat", side, k]
                before = stat[h, pl.ds(0, 1), :]
                top = jnp.maximum(before, top)
                kept = jnp.exp2(before - top)
            total, mixed = weigh(masked, top, codes, block_reader(functools.partial(pick, 1)))
            if carry:
                total = total + kept * stat[h, pl.ds(1, 1), :]
                mixed = mixed + kept * have["sum", side, k][h]
            if final:
                spare = results[-1]
                spare[i] = (mixed / total).astype(spare.dtype).T
                for shift in range(panel_size):
                    first_row = pl.multiple_of(lax.rem(panel + shift, panel_size) * piece, piece)
                    results[n * panel_size + shift][:, local] = spare[i, pl.ds(first_row, piece), :]
            else:
                sums, stats = results[2 * n : 2 * n + 2]
                sums[h] = mixed
                stats[h, pl.ds(0, 1), :] = top
                stats[h, pl.ds(1, 1), :] = total

        each_unit(sizes[k], unit)

    @pl.when(info_ref[0] == 1)
    def _():
        for n, entry in enumerate(jobs):
            job(n, *entry)


def assemble_kernel(panel_size, starts, sizes, aliased, info_ref, *refs):
    out_ref, sems = refs[-2:]
    refs = refs[1:] if aliased else refs
    count = len(sizes)
    width = out_ref.shape[1] // panel_size
    panel = info_ref[1]
    inner = info_ref[0] == 1
    copies = []
    for shift in range(panel_size):
        source = lax.rem(panel + panel_size - shift, panel_size)
        for chunk, (start, size) in enumerate(zip(starts, sizes)):
            columns = pl.ds(pl.multiple_of(source * width + start * HEAD_DIM, HEAD_DIM), size * HEAD_DIM)
            own, guest = (
                pltpu.make_async_copy(
                    refs[(side * count + chunk) * panel_size + shift],
                    out_ref.at[:, columns],
                    sems.at[shift, chunk],
                )
                for side in range(2)
            )
            pl.when(inner)(own.start)
            pl.when(jnp.logical_not(inner))(guest.start)
            copies.append(own)
    for copy in copies:
        copy.wait()


def relayed(queries, key_rows, value_rows, block_lists, block_counts, seq_size, panel_size):
    rows, width = queries.shape
    heads = width // HEAD_DIM
    chips = seq_size // CORES
    position = lax.axis_index("seq")
    panel = lax.axis_index("panel")
    chip, core = position // CORES, position % CORES
    last = chips - 1
    cores = range(CORES)
    inward = [(source * CORES + c, target * CORES + c) for source, target in ((0, 1), (last, last - 1)) for c in cores]
    across = [(source * CORES + c, target * CORES + c) for source, target in ((1, 2), (2, 1)) for c in cores]
    partner = [(z * CORES + c, z * CORES + CORES - 1 - c) for z in (1, 2) for c in cores]
    inner = [(z * CORES + c, z * CORES + c) for z in (1, 2) for c in cores]
    outward = [(target, source) for source, target in inward]
    in_vmem, in_smem, anywhere = (pl.BlockSpec(memory_space=s) for s in (pltpu.VMEM, pltpu.SMEM, pl.ANY))

    front = max(1, heads * FIRST_SHARE[0] // FIRST_SHARE[1])
    sizes = [front, heads - front]
    starts = [0, front]
    chunks = len(sizes)

    middle = [send(x, across) for x in (key_rows, value_rows)]

    def pack(chunk, *sources):
        return pl.pallas_call(
            functools.partial(pack_kernel, starts, sizes, chunk),
            out_shape=jax.ShapeDtypeStruct((len(sources) * rows, sizes[chunk] * HEAD_DIM), sources[0].dtype),
            in_specs=[anywhere] * len(sources),
            out_specs=in_vmem,
            scratch_shapes=[pltpu.SemaphoreType.DMA((len(sources),))],
            compiler_params=pltpu.CompilerParams(vmem_limit_bytes=VMEM_GRANT),
        )(*sources)

    packed = [pack(k, key_rows, value_rows) for k in range(chunks)]
    own_queries = [pack(k, queries) for k in range(chunks)]
    beside = [send(x, partner) for x in (key_rows, value_rows)]
    ends = [send(x, inward) for x in packed]
    guest_queries = [send(x, inward) for x in own_queries]
    middle_beside = [send(x, partner) for x in middle]

    is_inner = (chip >= 1) & (chip < last)
    end = jnp.where(chip * 2 < chips, 0, last)
    guest = end * CORES + core
    order = jnp.stack(
        [
            z * CORES + c
            for z in (chip, last - chip, end, last - end)
            for c in (core, CORES - 1 - core)
        ]
    )
    pick = (order[:, None] == jnp.arange(seq_size)).astype(jnp.int32)

    def arranged(owner):
        codes = tables(block_lists, block_counts, owner, seq_size)
        return jnp.concatenate([jnp.sum(codes[:, None, :seq_size] * pick, axis=2), codes[:, seq_size:]], axis=1)

    codes = jnp.stack([arranged(position), arranged(guest)]).reshape(-1)
    info = jnp.stack([is_inner.astype(jnp.int32), panel])

    ends_beside = [send(x, partner) for x in ends]
    far = [send(x, across) for x in ends]
    far_beside = [send(x, partner) for x in far]
    arrays = {}
    for slot, pair in ((1, beside), (2, middle), (3, middle_beside)):
        for kind in range(2):
            arrays["whole", slot, kind] = pair[kind]
    for k in range(chunks):
        arrays["query", 0, k], arrays["query", 1, k] = own_queries[k], guest_queries[k]
        for slot, parts in ((0, packed), (4, ends), (5, ends_beside), (6, far), (7, far_beside)):
            arrays["chunk", slot, k] = parts[k]

    own_pieces, guest_pieces = [], []
    both = ("seq", "panel")
    for name, jobs in STAGES:
        final = name.startswith("late")
        inputs = []
        for side, k, slots, carry in jobs:
            inputs.append(("query", side, k))
            for slot in slots:
                one = ("chunk", slot, k)
                inputs += [one] if one in arrays else [("whole", slot, kind) for kind in range(2)]
            if carry:
                inputs += [("sum", side, k), ("stat", side, k)]
        inputs = list(dict.fromkeys(inputs))
        if final:
            shapes = [
                jax.ShapeDtypeStruct((rows // panel_size, sizes[k] * HEAD_DIM), queries.dtype)
                for _, k, _, _ in jobs
                for _ in range(panel_size)
            ]
        else:
            shapes = [
                jax.ShapeDtypeStruct((sizes[k], height, rows), jnp.float32)
                for _, k, _, _ in jobs
                for height in (HEAD_DIM, 8)
            ]
        blocks = sum(sizes[k] * (len(slots) + (HOMES[side] in slots)) for side, k, slots, _ in jobs)
        results = pl.pallas_call(
            functools.partial(stage_kernel, seq_size, panel_size, heads, starts, sizes, jobs, inputs, final),
            out_shape=shapes,
            in_specs=[in_smem] * 2 + [in_vmem] * len(inputs),
            out_specs=[in_vmem] * len(shapes),
            scratch_shapes=[pltpu.VMEM((UNROLL, rows, HEAD_DIM), queries.dtype)] if final else [],
            compiler_params=pltpu.CompilerParams(vmem_limit_bytes=VMEM_GRANT),
            cost_estimate=pl.CostEstimate(
                flops=4 * rows * blocks * BLOCK * HEAD_DIM,
                bytes_accessed=blocks * 4 * BLOCK * HEAD_DIM,
                transcendentals=rows * blocks * BLOCK,
            ),
        )(info, codes, *(arrays[key] for key in inputs))
        if not final:
            for n, (side, k, _, _) in enumerate(jobs):
                arrays["sum", side, k], arrays["stat", side, k] = results[2 * n : 2 * n + 2]
            continue
        k = jobs[0][1]
        for shift in range(panel_size):
            mine, theirs = results[shift], results[panel_size + shift]
            if shift:
                mine = send(mine, pieces_of(inner, panel_size, shift), both)
            own_pieces.append(mine)
            guest_pieces.append(send(theirs, pieces_of(outward, panel_size, shift), both))

    split = (chunks - 1) * panel_size
    out = None
    for lo, hi, first, final in ((0, split, 0, chunks - 1), (split, chunks * panel_size, chunks - 1, chunks)):
        if lo == hi:
            continue
        pieces = own_pieces[lo:hi] + guest_pieces[lo:hi]
        before = [] if out is None else [out]
        out = pl.pallas_call(
            functools.partial(assemble_kernel, panel_size, starts[first:final], sizes[first:final], len(before)),
            out_shape=jax.ShapeDtypeStruct((rows // panel_size, width * panel_size), queries.dtype),
            in_specs=[in_smem] + [anywhere] * len(before) + [in_vmem] * len(pieces),
            out_specs=anywhere,
            scratch_shapes=[pltpu.SemaphoreType.DMA((panel_size, final - first))],
            input_output_aliases={1: 0} if before else {},
            compiler_params=pltpu.CompilerParams(vmem_limit_bytes=VMEM_GRANT),
        )(info, *before, *pieces)
    return out


def solution(mesh):
    seq_size, panel_size = mesh.shape["seq"], mesh.shape["panel"]
    relay = seq_size // CORES - 2 == 2
    if relay:
        body = functools.partial(relayed, seq_size=seq_size, panel_size=panel_size)
    else:
        body = functools.partial(gathered, seq_size=seq_size)
    return jax.shard_map(
        body,
        mesh=mesh,
        in_specs=(
            P(("groups", "seq"), "panel"),
            P(("groups", "seq"), "panel"),
            P(("groups", "seq"), "panel"),
            P("panel", None, None),
            P("panel", None),
        ),
        out_specs=P(("groups", "seq", "panel"), None),
        check_vma=False,
    )
```

```python
import functools

import jax
import jax.numpy as jnp
from jax import lax
from jax.experimental import pallas as pl
from jax.experimental.pallas import tpu as pltpu
from jax.sharding import PartitionSpec as P


HEAD_DIM = 128
BLOCK = 128
LOG2_E = 1.4426950408889634
DEAD = -1e30
CORES = 2
FIRST_SHARE = 7, 12
UNROLL = 5
VMEM_GRANT = 14 << 20
HOMES = 0, 4
STAGES = (
    ("early_0", ((0, 0, (0, 1), False), (0, 1, (0, 1), False))),
    ("early_1", ((0, 0, (2, 3, 4, 5), True), (0, 1, (2, 3), True))),
    ("early_2", ((1, 0, (0, 1, 2, 3, 4, 5), False),)),
    ("early_3", ((1, 1, (0, 1, 2, 3, 4, 5), False), (0, 1, (4, 5), True))),
    ("late_0", ((1, 0, (6, 7), True),)),
    ("late_3", ((0, 0, (6, 7), True),)),
    ("late_1", ((1, 1, (6, 7), True),)),
    ("late_2", ((0, 1, (6, 7), True),)),
)


def tables(block_lists, block_counts, owner, seq_size):
    heads, tiles, listed = block_lists.shape
    per_index = tiles // seq_size
    lists = lax.dynamic_slice_in_dim(block_lists, owner * per_index, per_index, 1)
    counts = lax.dynamic_slice_in_dim(block_counts, owner * per_index, per_index, 1)
    slot_live = jnp.arange(listed, dtype=jnp.int32) < counts[:, :, None]
    ids = jnp.arange(tiles, dtype=jnp.int32)
    hits = (lists[:, :, :, None] == ids) & slot_live[:, :, :, None]
    keep = jnp.any(hits, axis=2).astype(jnp.int32).reshape(heads, per_index, seq_size, per_index)
    low, high = keep[..., 0], keep[..., 1]
    taken = jnp.max(high, axis=1)
    live = jnp.where(taken[:, None, :] == 1, high, low)
    other = jnp.where(taken[:, None, :] == 1, low, high)
    bits = jnp.array([2 << tile for tile in range(per_index)], jnp.int32)[None, :, None]
    code = taken + jnp.sum(live * bits, axis=1)
    code_other = (1 - taken) + jnp.sum(other * bits, axis=1)
    mine = jnp.arange(seq_size) == owner
    extra = jnp.sum(jnp.where(mine, code_other, 0), axis=1, keepdims=True)
    return jnp.concatenate([code, extra], axis=1)


def attend(query, codes, key_block, value_block):
    rows = query.shape[0]
    factor = HEAD_DIM ** (-0.5) * LOG2_E
    masked = []
    for j, code in enumerate(codes):
        scores = lax.dot_general(
            query, key_block(j, code & 1), (((1,), (1,)), ((), ())), preferred_element_type=jnp.float32
        )
        parts = []
        for tile in range(rows // BLOCK):
            bias = jnp.where((code >> (tile + 1)) & 1 == 1, 0.0, DEAD).astype(jnp.float32)
            parts.append(scores[tile * BLOCK : (tile + 1) * BLOCK] * factor + bias)
        masked.append(jnp.concatenate(parts, axis=0))
    top = jnp.max(functools.reduce(jnp.maximum, masked), axis=1, keepdims=True)
    total, mixed = None, None
    for j, code in enumerate(codes):
        weights = jnp.exp2(masked[j] - top)
        total = weights if total is None else total + weights
        product = jnp.dot(
            weights.astype(jnp.bfloat16), value_block(j, code & 1), preferred_element_type=jnp.float32
        )
        mixed = product if mixed is None else mixed + product
    return mixed / jnp.sum(total, axis=1, keepdims=True)


def gathered_kernel(seq_size, own_rows, info_ref, code_ref, query_ref, key_ref, value_ref, out_ref):
    head = pl.program_id(0)
    owner = info_ref[0]

    def block(ref):
        def read(j, which):
            index = owner if j == seq_size else j
            return ref[pl.ds(pl.multiple_of(index * own_rows + which * BLOCK, BLOCK), BLOCK), :]

        return read

    codes = [code_ref[head * (seq_size + 1) + j] for j in range(seq_size + 1)]
    out_ref[...] = attend(query_ref[...], codes, block(key_ref), block(value_ref)).astype(out_ref.dtype)


def gathered(queries, key_rows, value_rows, block_lists, block_counts, seq_size):
    rows, width = queries.shape
    heads = width // HEAD_DIM
    position = lax.axis_index("seq")
    keys = lax.all_gather(key_rows, "seq", axis=0, tiled=True)
    values = lax.all_gather(value_rows, "seq", axis=0, tiled=True)
    codes = tables(block_lists, block_counts, position, seq_size).reshape(-1)
    all_rows = keys.shape[0]
    out = pl.pallas_call(
        functools.partial(gathered_kernel, seq_size, rows),
        out_shape=jax.ShapeDtypeStruct((rows, width), queries.dtype),
        grid_spec=pltpu.PrefetchScalarGridSpec(
            num_scalar_prefetch=2,
            grid=(heads,),
            in_specs=[
                pl.BlockSpec((rows, HEAD_DIM), lambda h, *_: (0, h)),
                pl.BlockSpec((all_rows, HEAD_DIM), lambda h, *_: (0, h)),
                pl.BlockSpec((all_rows, HEAD_DIM), lambda h, *_: (0, h)),
            ],
            out_specs=pl.BlockSpec((rows, HEAD_DIM), lambda h, *_: (0, h)),
        ),
        name="attend_gathered",
    )(position.reshape(1), codes, queries, keys, values)
    return lax.all_to_all(out, "panel", split_axis=0, concat_axis=1, tiled=True)


def pieces_of(seq_pairs, panel_size, shift):
    return [
        (source * panel_size + panel, target * panel_size + (panel + shift) % panel_size)
        for source, target in seq_pairs
        for panel in range(panel_size)
    ]


def send(value, pairs, axes="seq"):
    return lax.ppermute(value, axes, pairs)


def pack_kernel(starts, sizes, chunk, *refs):
    sources, out, sems = refs[:-2], refs[-2], refs[-1]
    rows = sources[0].shape[0]
    columns = pl.ds(starts[chunk] * HEAD_DIM, sizes[chunk] * HEAD_DIM)
    copies = [
        pltpu.make_async_copy(ref.at[:, columns], out.at[pl.ds(kind * rows, rows), :], sems.at[kind])
        for kind, ref in enumerate(sources)
    ]
    for copy in copies:
        copy.start()
    for copy in copies:
        copy.wait()


def masked_scores(query, codes, key_block):
    factor = HEAD_DIM ** (-0.5) * LOG2_E
    masked = []
    for j, code in codes:
        scores = lax.dot_general(
            key_block(j, code & 1), query, (((1,), (1,)), ((), ())), preferred_element_type=jnp.float32
        )
        tiles = query.shape[0] // BLOCK
        bias = [
            jnp.full((1, BLOCK), jnp.where((code >> (tile + 1)) & 1 == 1, 0.0, DEAD), jnp.float32)
            for tile in range(tiles)
        ]
        masked.append(scores * factor + jnp.concatenate(bias, axis=1))
    return masked


def weigh(masked, top, codes, value_block):
    total, mixed = None, None
    for scores, (j, code) in zip(masked, codes):
        weights = jnp.exp2(scores - top)
        total = weights if total is None else total + weights
        product = lax.dot_general(
            value_block(j, code & 1),
            weights.astype(jnp.bfloat16),
            (((0,), (0,)), ((), ())),
            preferred_element_type=jnp.float32,
        )
        mixed = product if mixed is None else mixed + product
    return jnp.sum(total, axis=0, keepdims=True), mixed


def highest(masked):
    return jnp.max(functools.reduce(jnp.maximum, masked), axis=0, keepdims=True)


def each_unit(count, unit):
    groups = -(-count // UNROLL)
    size = -(-count // groups)
    whole = count // size

    @pl.loop(0, whole)
    def _(group):
        for i in range(size):
            unit(group * size, i)

    for i in range(count - whole * size):
        unit(whole * size, i)


def columns_of(head):
    return pl.ds(pl.multiple_of(head * HEAD_DIM, HEAD_DIM), HEAD_DIM)


def block_reader(pick):
    def block(slot, which):
        ref, first, columns = pick(slot)
        return ref[pl.ds(pl.multiple_of(first + which * BLOCK, BLOCK), BLOCK), columns]

    return block


def stage_kernel(seq_size, panel_size, heads, starts, sizes, jobs, inputs, final, *refs):
    info_ref, code_ref = refs[:2]
    have = dict(zip(inputs, refs[2:]))
    results = refs[2 + len(inputs) :]
    panel = info_ref[1]

    def job(n, side, k, slots, carry):
        queries = have["query", side, k]
        rows = queries.shape[0]
        piece = rows // panel_size

        def unit(base, i):
            h = base + i
            local = columns_of(h)
            first = (side * heads + h + starts[k]) * (seq_size + 1)
            codes = [(slot, code_ref[first + slot]) for slot in slots]
            if HOMES[side] in slots:
                codes.append((HOMES[side], code_ref[first + seq_size]))

            def pick(kind, slot):
                if ("chunk", slot, k) in have:
                    return have["chunk", slot, k], kind * rows, local
                return have["whole", slot, kind], 0, columns_of(h + starts[k])

            masked = masked_scores(queries[:, local], codes, block_reader(functools.partial(pick, 0)))
            top = highest(masked)
            if carry:
                stat = have["stat", side, k]
                before = stat[h, pl.ds(0, 1), :]
                top = jnp.maximum(before, top)
                kept = jnp.exp2(before - top)
            total, mixed = weigh(masked, top, codes, block_reader(functools.partial(pick, 1)))
            if carry:
                total = total + kept * stat[h, pl.ds(1, 1), :]
                mixed = mixed + kept * have["sum", side, k][h]
            if final:
                spare = results[-1]
                spare[i] = (mixed / total).astype(spare.dtype).T
                for shift in range(panel_size):
                    first_row = pl.multiple_of(lax.rem(panel + shift, panel_size) * piece, piece)
                    results[n * panel_size + shift][:, local] = spare[i, pl.ds(first_row, piece), :]
            else:
                sums, stats = results[2 * n : 2 * n + 2]
                sums[h] = mixed
                stats[h, pl.ds(0, 1), :] = top
                stats[h, pl.ds(1, 1), :] = total

        each_unit(sizes[k], unit)

    @pl.when(info_ref[0] == 1)
    def _():
        for n, entry in enumerate(jobs):
            job(n, *entry)


def assemble_kernel(panel_size, starts, sizes, aliased, info_ref, *refs):
    out_ref, sems = refs[-2:]
    refs = refs[1:] if aliased else refs
    count = len(sizes)
    width = out_ref.shape[1] // panel_size
    panel = info_ref[1]
    inner = info_ref[0] == 1
    copies = []
    for shift in range(panel_size):
        source = lax.rem(panel + panel_size - shift, panel_size)
        for chunk, (start, size) in enumerate(zip(starts, sizes)):
            columns = pl.ds(pl.multiple_of(source * width + start * HEAD_DIM, HEAD_DIM), size * HEAD_DIM)
            own, guest = (
                pltpu.make_async_copy(
                    refs[(side * count + chunk) * panel_size + shift],
                    out_ref.at[:, columns],
                    sems.at[shift, chunk],
                )
                for side in range(2)
            )
            pl.when(inner)(own.start)
            pl.when(jnp.logical_not(inner))(guest.start)
            copies.append(own)
    for copy in copies:
        copy.wait()


def relayed(queries, key_rows, value_rows, block_lists, block_counts, seq_size, panel_size):
    rows, width = queries.shape
    heads = width // HEAD_DIM
    chips = seq_size // CORES
    position = lax.axis_index("seq")
    panel = lax.axis_index("panel")
    chip, core = position // CORES, position % CORES
    last = chips - 1
    cores = range(CORES)
    inward = [(source * CORES + c, target * CORES + c) for source, target in ((0, 1), (last, last - 1)) for c in cores]
    across = [(source * CORES + c, target * CORES + c) for source, target in ((1, 2), (2, 1)) for c in cores]
    partner = [(z * CORES + c, z * CORES + CORES - 1 - c) for z in (1, 2) for c in cores]
    inner = [(z * CORES + c, z * CORES + c) for z in (1, 2) for c in cores]
    outward = [(target, source) for source, target in inward]
    in_vmem, in_smem, anywhere = (pl.BlockSpec(memory_space=s) for s in (pltpu.VMEM, pltpu.SMEM, pl.ANY))

    front = max(1, heads * FIRST_SHARE[0] // FIRST_SHARE[1])
    sizes = [front, heads - front]
    starts = [0, front]
    chunks = len(sizes)

    middle = [send(x, across) for x in (key_rows, value_rows)]

    def pack(chunk, *sources):
        return pl.pallas_call(
            functools.partial(pack_kernel, starts, sizes, chunk),
            out_shape=jax.ShapeDtypeStruct((len(sources) * rows, sizes[chunk] * HEAD_DIM), sources[0].dtype),
            in_specs=[anywhere] * len(sources),
            out_specs=in_vmem,
            scratch_shapes=[pltpu.SemaphoreType.DMA((len(sources),))],
            compiler_params=pltpu.CompilerParams(vmem_limit_bytes=VMEM_GRANT),
        )(*sources)

    packed = [pack(k, key_rows, value_rows) for k in range(chunks)]
    own_queries = [pack(k, queries) for k in range(chunks)]
    beside = [send(x, partner) for x in (key_rows, value_rows)]
    ends = [send(x, inward) for x in packed]
    guest_queries = [send(x, inward) for x in own_queries]
    middle_beside = [send(x, partner) for x in middle]

    is_inner = (chip >= 1) & (chip < last)
    end = jnp.where(chip * 2 < chips, 0, last)
    guest = end * CORES + core
    order = jnp.stack(
        [
            z * CORES + c
            for z in (chip, last - chip, end, last - end)
            for c in (core, CORES - 1 - core)
        ]
    )
    pick = (order[:, None] == jnp.arange(seq_size)).astype(jnp.int32)

    def arranged(owner):
        codes = tables(block_lists, block_counts, owner, seq_size)
        return jnp.concatenate([jnp.sum(codes[:, None, :seq_size] * pick, axis=2), codes[:, seq_size:]], axis=1)

    codes = jnp.stack([arranged(position), arranged(guest)]).reshape(-1)
    info = jnp.stack([is_inner.astype(jnp.int32), panel])

    ends_beside = [send(x, partner) for x in ends]
    far = [send(x, across) for x in ends]
    far_beside = [send(x, partner) for x in far]
    arrays = {}
    for slot, pair in ((1, beside), (2, middle), (3, middle_beside)):
        for kind in range(2):
            arrays["whole", slot, kind] = pair[kind]
    for k in range(chunks):
        arrays["query", 0, k], arrays["query", 1, k] = own_queries[k], guest_queries[k]
        for slot, parts in ((0, packed), (4, ends), (5, ends_beside), (6, far), (7, far_beside)):
            arrays["chunk", slot, k] = parts[k]

    pieces = {}
    both = ("seq", "panel")
    for name, jobs in STAGES:
        final = name.startswith("late")
        inputs = []
        for side, k, slots, carry in jobs:
            inputs.append(("query", side, k))
            for slot in slots:
                one = ("chunk", slot, k)
                inputs += [one] if one in arrays else [("whole", slot, kind) for kind in range(2)]
            if carry:
                inputs += [("sum", side, k), ("stat", side, k)]
        inputs = list(dict.fromkeys(inputs))
        if final:
            shapes = [
                jax.ShapeDtypeStruct((rows // panel_size, sizes[k] * HEAD_DIM), queries.dtype)
                for _, k, _, _ in jobs
                for _ in range(panel_size)
            ]
        else:
            shapes = [
                jax.ShapeDtypeStruct((sizes[k], height, rows), jnp.float32)
                for _, k, _, _ in jobs
                for height in (HEAD_DIM, 8)
            ]
        blocks = sum(sizes[k] * (len(slots) + (HOMES[side] in slots)) for side, k, slots, _ in jobs)
        results = pl.pallas_call(
            functools.partial(stage_kernel, seq_size, panel_size, heads, starts, sizes, jobs, inputs, final),
            out_shape=shapes,
            in_specs=[in_smem] * 2 + [in_vmem] * len(inputs),
            out_specs=[in_vmem] * len(shapes),
            scratch_shapes=[pltpu.VMEM((UNROLL, rows, HEAD_DIM), queries.dtype)] if final else [],
            compiler_params=pltpu.CompilerParams(vmem_limit_bytes=VMEM_GRANT),
            cost_estimate=pl.CostEstimate(
                flops=4 * rows * blocks * BLOCK * HEAD_DIM,
                bytes_accessed=blocks * 4 * BLOCK * HEAD_DIM,
                transcendentals=rows * blocks * BLOCK,
            ),
        )(info, codes, *(arrays[key] for key in inputs))
        if not final:
            for n, (side, k, _, _) in enumerate(jobs):
                arrays["sum", side, k], arrays["stat", side, k] = results[2 * n : 2 * n + 2]
            continue
        for n, (side, k, _, _) in enumerate(jobs):
            for shift in range(panel_size):
                piece = results[n * panel_size + shift]
                if side == 1:
                    piece = send(piece, pieces_of(outward, panel_size, shift), both)
                elif shift:
                    piece = send(piece, pieces_of(inner, panel_size, shift), both)
                pieces[side, k, shift] = piece

    out = None
    for first, final in ((0, chunks - 1), (chunks - 1, chunks)):
        parts = [
            pieces[side, k, shift] for side in range(2) for k in range(first, final) for shift in range(panel_size)
        ]
        before = [] if out is None else [out]
        out = pl.pallas_call(
            functools.partial(assemble_kernel, panel_size, starts[first:final], sizes[first:final], len(before)),
            out_shape=jax.ShapeDtypeStruct((rows // panel_size, width * panel_size), queries.dtype),
            in_specs=[in_smem] + [anywhere] * len(before) + [in_vmem] * len(parts),
            out_specs=anywhere,
            scratch_shapes=[pltpu.SemaphoreType.DMA((panel_size, final - first))],
            input_output_aliases={1: 0} if before else {},
            compiler_params=pltpu.CompilerParams(vmem_limit_bytes=VMEM_GRANT),
        )(info, *before, *parts)
    return out


def solution(mesh):
    seq_size, panel_size = mesh.shape["seq"], mesh.shape["panel"]
    relay = seq_size // CORES - 2 == 2
    if relay:
        body = functools.partial(relayed, seq_size=seq_size, panel_size=panel_size)
    else:
        body = functools.partial(gathered, seq_size=seq_size)
    return jax.shard_map(
        body,
        mesh=mesh,
        in_specs=(
            P(("groups", "seq"), "panel"),
            P(("groups", "seq"), "panel"),
            P(("groups", "seq"), "panel"),
            P("panel", None, None),
            P("panel", None),
        ),
        out_specs=P(("groups", "seq", "panel"), None),
        check_vma=False,
    )
```

```python
import functools

import jax
import jax.numpy as jnp
from jax import lax
from jax.experimental import pallas as pl
from jax.experimental.pallas import tpu as pltpu
from jax.sharding import PartitionSpec as P


HEAD_DIM = 128
BLOCK = 128
LOG2_E = 1.4426950408889634
DEAD = -1e30
CORES = 2
FIRST_SHARE = 7, 12
UNROLL = 7
VMEM_GRANT = 14 << 20
HOMES = 0, 4
STAGES = (
    ("early_0", ((0, 0, (0, 1), False), (0, 1, (0, 1), False)), ()),
    ("early_1", ((0, 0, (2, 3, 4, 5), True), (0, 1, (2, 3), True)), ()),
    (
        "early_2",
        ((1, 0, (0, 1, 2, 3, 4, 5), False),),
        (("chunk", 1, 1), ("chunk", 2, 1), ("chunk", 3, 1), ("query", 1, 0)),
    ),
    ("early_3", ((1, 1, (0, 1, 2, 3, 4, 5), False),), (("query", 1, 1),)),
    ("late_0", ((1, 0, (6, 7), True),), ()),
    ("late_3", ((0, 0, (6, 7), True),), ()),
    ("early_4", ((0, 1, (4, 5), True),), ()),
    ("late_1", ((1, 1, (6, 7), True),), ()),
    ("late_2", ((0, 1, (6, 7), True),), ()),
)


def tables(block_lists, block_counts, owner, seq_size):
    heads, tiles, listed = block_lists.shape
    per_index = tiles // seq_size
    lists = lax.dynamic_slice_in_dim(block_lists, owner * per_index, per_index, 1)
    counts = lax.dynamic_slice_in_dim(block_counts, owner * per_index, per_index, 1)
    slot_live = jnp.arange(listed, dtype=jnp.int32) < counts[:, :, None]
    ids = jnp.arange(tiles, dtype=jnp.int32)
    hits = (lists[:, :, :, None] == ids) & slot_live[:, :, :, None]
    keep = jnp.any(hits, axis=2).astype(jnp.int32).reshape(heads, per_index, seq_size, per_index)
    low, high = keep[..., 0], keep[..., 1]
    taken = jnp.max(high, axis=1)
    live = jnp.where(taken[:, None, :] == 1, high, low)
    other = jnp.where(taken[:, None, :] == 1, low, high)
    bits = jnp.array([2 << tile for tile in range(per_index)], jnp.int32)[None, :, None]
    code = taken + jnp.sum(live * bits, axis=1)
    code_other = (1 - taken) + jnp.sum(other * bits, axis=1)
    mine = jnp.arange(seq_size) == owner
    extra = jnp.sum(jnp.where(mine, code_other, 0), axis=1, keepdims=True)
    return jnp.concatenate([code, extra], axis=1)


def attend(query, codes, key_block, value_block):
    rows = query.shape[0]
    factor = HEAD_DIM ** (-0.5) * LOG2_E
    masked = []
    for j, code in enumerate(codes):
        scores = lax.dot_general(
            query, key_block(j, code & 1), (((1,), (1,)), ((), ())), preferred_element_type=jnp.float32
        )
        parts = []
        for tile in range(rows // BLOCK):
            bias = jnp.where((code >> (tile + 1)) & 1 == 1, 0.0, DEAD).astype(jnp.float32)
            parts.append(scores[tile * BLOCK : (tile + 1) * BLOCK] * factor + bias)
        masked.append(jnp.concatenate(parts, axis=0))
    top = jnp.max(functools.reduce(jnp.maximum, masked), axis=1, keepdims=True)
    total, mixed = None, None
    for j, code in enumerate(codes):
        weights = jnp.exp2(masked[j] - top)
        total = weights if total is None else total + weights
        product = jnp.dot(
            weights.astype(jnp.bfloat16), value_block(j, code & 1), preferred_element_type=jnp.float32
        )
        mixed = product if mixed is None else mixed + product
    return mixed / jnp.sum(total, axis=1, keepdims=True)


def gathered_kernel(seq_size, own_rows, info_ref, code_ref, query_ref, key_ref, value_ref, out_ref):
    head = pl.program_id(0)
    owner = info_ref[0]

    def block(ref):
        def read(j, which):
            index = owner if j == seq_size else j
            return ref[pl.ds(pl.multiple_of(index * own_rows + which * BLOCK, BLOCK), BLOCK), :]

        return read

    codes = [code_ref[head * (seq_size + 1) + j] for j in range(seq_size + 1)]
    out_ref[...] = attend(query_ref[...], codes, block(key_ref), block(value_ref)).astype(out_ref.dtype)


def gathered(queries, key_rows, value_rows, block_lists, block_counts, seq_size):
    rows, width = queries.shape
    heads = width // HEAD_DIM
    position = lax.axis_index("seq")
    keys = lax.all_gather(key_rows, "seq", axis=0, tiled=True)
    values = lax.all_gather(value_rows, "seq", axis=0, tiled=True)
    codes = tables(block_lists, block_counts, position, seq_size).reshape(-1)
    all_rows = keys.shape[0]
    out = pl.pallas_call(
        functools.partial(gathered_kernel, seq_size, rows),
        out_shape=jax.ShapeDtypeStruct((rows, width), queries.dtype),
        grid_spec=pltpu.PrefetchScalarGridSpec(
            num_scalar_prefetch=2,
            grid=(heads,),
            in_specs=[
                pl.BlockSpec((rows, HEAD_DIM), lambda h, *_: (0, h)),
                pl.BlockSpec((all_rows, HEAD_DIM), lambda h, *_: (0, h)),
                pl.BlockSpec((all_rows, HEAD_DIM), lambda h, *_: (0, h)),
            ],
            out_specs=pl.BlockSpec((rows, HEAD_DIM), lambda h, *_: (0, h)),
        ),
        name="attend_gathered",
    )(position.reshape(1), codes, queries, keys, values)
    return lax.all_to_all(out, "panel", split_axis=0, concat_axis=1, tiled=True)


def pieces_of(seq_pairs, panel_size, shift):
    return [
        (source * panel_size + panel, target * panel_size + (panel + shift) % panel_size)
        for source, target in seq_pairs
        for panel in range(panel_size)
    ]


def send(value, pairs, axes="seq"):
    return lax.ppermute(value, axes, pairs)


def pack_kernel(starts, sizes, chunk, *refs):
    sources, out, sems = refs[:-2], refs[-2], refs[-1]
    rows = sources[0].shape[0]
    columns = pl.ds(starts[chunk] * HEAD_DIM, sizes[chunk] * HEAD_DIM)
    copies = [
        pltpu.make_async_copy(ref.at[:, columns], out.at[pl.ds(kind * rows, rows), :], sems.at[kind])
        for kind, ref in enumerate(sources)
    ]
    for copy in copies:
        copy.start()
    for copy in copies:
        copy.wait()


def masked_scores(query, codes, key_block):
    factor = HEAD_DIM ** (-0.5) * LOG2_E
    masked = []
    for j, code in codes:
        scores = lax.dot_general(
            key_block(j, code & 1), query, (((1,), (1,)), ((), ())), preferred_element_type=jnp.float32
        )
        tiles = query.shape[0] // BLOCK
        bias = [
            jnp.full((1, BLOCK), jnp.where((code >> (tile + 1)) & 1 == 1, 0.0, DEAD), jnp.float32)
            for tile in range(tiles)
        ]
        masked.append(scores * factor + jnp.concatenate(bias, axis=1))
    return masked


def weigh(masked, top, codes, value_block):
    total, mixed = None, None
    for scores, (j, code) in zip(masked, codes):
        weights = jnp.exp2(scores - top)
        total = weights if total is None else total + weights
        product = lax.dot_general(
            value_block(j, code & 1),
            weights.astype(jnp.bfloat16),
            (((0,), (0,)), ((), ())),
            preferred_element_type=jnp.float32,
        )
        mixed = product if mixed is None else mixed + product
    return jnp.sum(total, axis=0, keepdims=True), mixed


def highest(masked):
    return jnp.max(functools.reduce(jnp.maximum, masked), axis=0, keepdims=True)


def each_unit(count, unit):
    groups = -(-count // UNROLL)
    size = -(-count // groups)
    whole = count // size

    @pl.loop(0, whole)
    def _(group):
        for i in range(size):
            unit(group * size, i)

    for i in range(count - whole * size):
        unit(whole * size, i)


def columns_of(head):
    return pl.ds(pl.multiple_of(head * HEAD_DIM, HEAD_DIM), HEAD_DIM)


def block_reader(pick):
    def block(slot, which):
        ref, first, columns = pick(slot)
        return ref[pl.ds(pl.multiple_of(first + which * BLOCK, BLOCK), BLOCK), columns]

    return block


def stage_kernel(seq_size, panel_size, heads, starts, sizes, jobs, keeps, inputs, final, *refs):
    info_ref, code_ref = refs[:2]
    have = dict(zip(inputs, refs[2:]))
    results = refs[2 + len(inputs) :]
    panel = info_ref[1]

    def job(n, side, k, slots, carry):
        queries = have["query", side, k]
        rows = queries.shape[0]
        piece = rows // panel_size

        def unit(base, i):
            h = base + i
            local = columns_of(h)
            first = (side * heads + h + starts[k]) * (seq_size + 1)
            codes = [(slot, code_ref[first + slot]) for slot in slots]
            if HOMES[side] in slots:
                codes.append((HOMES[side], code_ref[first + seq_size]))

            def pick(kind, slot):
                if ("chunk", slot, k) in have:
                    return have["chunk", slot, k], kind * rows, local
                return have["whole", slot, kind], 0, columns_of(h + starts[k])

            masked = masked_scores(queries[:, local], codes, block_reader(functools.partial(pick, 0)))
            top = highest(masked)
            if carry:
                stat = have["stat", side, k]
                before = stat[h, pl.ds(0, 1), :]
                top = jnp.maximum(before, top)
                kept = jnp.exp2(before - top)
            total, mixed = weigh(masked, top, codes, block_reader(functools.partial(pick, 1)))
            if carry:
                total = total + kept * stat[h, pl.ds(1, 1), :]
                mixed = mixed + kept * have["sum", side, k][h]
            if final:
                spare = results[-1]
                spare[i] = (mixed * (1.0 / total)).astype(spare.dtype).T
                for shift in range(panel_size):
                    first_row = pl.multiple_of(lax.rem(panel + shift, panel_size) * piece, piece)
                    results[n * panel_size + shift][:, local] = spare[i, pl.ds(first_row, piece), :]
            else:
                sums, stats = results[2 * n : 2 * n + 2]
                sums[h] = mixed
                stats[h, pl.ds(0, 1), :] = top
                stats[h, pl.ds(1, 1), :] = total

        each_unit(sizes[k], unit)

    @pl.when(info_ref[0] == 1)
    def _():
        for n, entry in enumerate(jobs):
            job(n, *entry)
        for n, (kind, which, k) in enumerate(keeps):
            copy = results[2 * len(jobs) + n]
            if kind == "query":
                copy[...] = have[kind, which, k][...]
                continue
            rows = copy.shape[0] // 2
            columns = pl.ds(starts[k] * HEAD_DIM, sizes[k] * HEAD_DIM)
            for half in range(2):
                copy[pl.ds(half * rows, rows), :] = have["whole", which, half][:, columns]


def assemble_kernel(panel_size, starts, sizes, aliased, info_ref, *refs):
    out_ref, sems = refs[-2:]
    refs = refs[1:] if aliased else refs
    count = len(sizes)
    width = out_ref.shape[1] // panel_size
    panel = info_ref[1]
    inner = info_ref[0] == 1
    copies = []
    for shift in range(panel_size):
        source = lax.rem(panel + panel_size - shift, panel_size)
        for chunk, (start, size) in enumerate(zip(starts, sizes)):
            columns = pl.ds(pl.multiple_of(source * width + start * HEAD_DIM, HEAD_DIM), size * HEAD_DIM)
            own, guest = (
                pltpu.make_async_copy(
                    refs[(side * count + chunk) * panel_size + shift],
                    out_ref.at[:, columns],
                    sems.at[shift, chunk],
                )
                for side in range(2)
            )
            pl.when(inner)(own.start)
            pl.when(jnp.logical_not(inner))(guest.start)
            copies.append(own)
    for copy in copies:
        copy.wait()


def relayed(queries, key_rows, value_rows, block_lists, block_counts, seq_size, panel_size):
    rows, width = queries.shape
    heads = width // HEAD_DIM
    chips = seq_size // CORES
    position = lax.axis_index("seq")
    panel = lax.axis_index("panel")
    chip, core = position // CORES, position % CORES
    last = chips - 1
    cores = range(CORES)
    inward = [(source * CORES + c, target * CORES + c) for source, target in ((0, 1), (last, last - 1)) for c in cores]
    across = [(source * CORES + c, target * CORES + c) for source, target in ((1, 2), (2, 1)) for c in cores]
    partner = [(z * CORES + c, z * CORES + CORES - 1 - c) for z in (1, 2) for c in cores]
    inner = [(z * CORES + c, z * CORES + c) for z in (1, 2) for c in cores]
    outward = [(target, source) for source, target in inward]
    in_vmem, in_smem, anywhere = (pl.BlockSpec(memory_space=s) for s in (pltpu.VMEM, pltpu.SMEM, pl.ANY))

    front = max(1, heads * FIRST_SHARE[0] // FIRST_SHARE[1])
    sizes = [front, heads - front]
    starts = [0, front]
    chunks = len(sizes)

    middle = [send(x, across) for x in (key_rows, value_rows)]

    def pack(chunk, *sources):
        return pl.pallas_call(
            functools.partial(pack_kernel, starts, sizes, chunk),
            out_shape=jax.ShapeDtypeStruct((len(sources) * rows, sizes[chunk] * HEAD_DIM), sources[0].dtype),
            in_specs=[anywhere] * len(sources),
            out_specs=in_vmem,
            scratch_shapes=[pltpu.SemaphoreType.DMA((len(sources),))],
            compiler_params=pltpu.CompilerParams(vmem_limit_bytes=VMEM_GRANT),
        )(*sources)

    packed = [pack(k, key_rows, value_rows) for k in range(chunks)]
    own_queries = [pack(k, queries) for k in range(chunks)]
    beside = [send(x, partner) for x in (key_rows, value_rows)]
    ends = [send(x, inward) for x in packed]
    guest_queries = [send(x, inward) for x in own_queries]
    middle_beside = [send(x, partner) for x in middle]

    is_inner = (chip >= 1) & (chip < last)
    end = jnp.where(chip * 2 < chips, 0, last)
    guest = end * CORES + core
    order = jnp.stack(
        [
            z * CORES + c
            for z in (chip, last - chip, end, last - end)
            for c in (core, CORES - 1 - core)
        ]
    )
    pick = (order[:, None] == jnp.arange(seq_size)).astype(jnp.int32)

    def arranged(owner):
        codes = tables(block_lists, block_counts, owner, seq_size)
        return jnp.concatenate([jnp.sum(codes[:, None, :seq_size] * pick, axis=2), codes[:, seq_size:]], axis=1)

    codes = jnp.stack([arranged(position), arranged(guest)]).reshape(-1)
    info = jnp.stack([is_inner.astype(jnp.int32), panel])

    ends_beside = [send(x, partner) for x in ends]
    far = [send(x, across) for x in ends]
    far_beside = [send(x, partner) for x in far]
    arrays = {}
    for slot, pair in ((1, beside), (2, middle), (3, middle_beside)):
        for kind in range(2):
            arrays["whole", slot, kind] = pair[kind]
    for k in range(chunks):
        arrays["query", 0, k], arrays["query", 1, k] = own_queries[k], guest_queries[k]
        for slot, parts in ((0, packed), (4, ends), (5, ends_beside), (6, far), (7, far_beside)):
            arrays["chunk", slot, k] = parts[k]

    pieces = {}
    both = ("seq", "panel")
    for name, jobs, keeps in STAGES:
        final = name.startswith("late")
        inputs = []
        for side, k, slots, carry in jobs:
            inputs.append(("query", side, k))
            for slot in slots:
                one = ("chunk", slot, k)
                inputs += [one] if one in arrays else [("whole", slot, kind) for kind in range(2)]
            if carry:
                inputs += [("sum", side, k), ("stat", side, k)]
        inputs = list(dict.fromkeys(inputs))
        if final:
            shapes = [
                jax.ShapeDtypeStruct((rows // panel_size, sizes[k] * HEAD_DIM), queries.dtype)
                for _, k, _, _ in jobs
                for _ in range(panel_size)
            ]
        else:
            shapes = [
                jax.ShapeDtypeStruct((sizes[k], height, rows), jnp.float32)
                for _, k, _, _ in jobs
                for height in (HEAD_DIM, 8)
            ]
            shapes += [
                jax.ShapeDtypeStruct(((1 if kind == "query" else 2) * rows, sizes[k] * HEAD_DIM), queries.dtype)
                for kind, _, k in keeps
            ]
        blocks = sum(sizes[k] * (len(slots) + (HOMES[side] in slots)) for side, k, slots, _ in jobs)
        results = pl.pallas_call(
            functools.partial(stage_kernel, seq_size, panel_size, heads, starts, sizes, jobs, keeps, inputs, final),
            out_shape=shapes,
            in_specs=[in_smem] * 2 + [in_vmem] * len(inputs),
            out_specs=[in_vmem] * len(shapes),
            scratch_shapes=[pltpu.VMEM((UNROLL, rows, HEAD_DIM), queries.dtype)] if final else [],
            compiler_params=pltpu.CompilerParams(vmem_limit_bytes=VMEM_GRANT),
            cost_estimate=pl.CostEstimate(
                flops=4 * rows * blocks * BLOCK * HEAD_DIM,
                bytes_accessed=blocks * 4 * BLOCK * HEAD_DIM,
                transcendentals=rows * blocks * BLOCK,
            ),
        )(info, codes, *(arrays[key] for key in inputs))
        if not final:
            for n, (side, k, _, _) in enumerate(jobs):
                arrays["sum", side, k], arrays["stat", side, k] = results[2 * n : 2 * n + 2]
            arrays.update(zip(keeps, results[2 * len(jobs) :]))
            continue
        for n, (side, k, _, _) in enumerate(jobs):
            for shift in range(panel_size):
                piece = results[n * panel_size + shift]
                if side == 1:
                    piece = send(piece, pieces_of(outward, panel_size, shift), both)
                elif shift:
                    piece = send(piece, pieces_of(inner, panel_size, shift), both)
                pieces[side, k, shift] = piece

    out = None
    for first, final in ((0, chunks - 1), (chunks - 1, chunks)):
        parts = [
            pieces[side, k, shift] for side in range(2) for k in range(first, final) for shift in range(panel_size)
        ]
        before = [] if out is None else [out]
        out = pl.pallas_call(
            functools.partial(assemble_kernel, panel_size, starts[first:final], sizes[first:final], len(before)),
            out_shape=jax.ShapeDtypeStruct((rows // panel_size, width * panel_size), queries.dtype),
            in_specs=[in_smem] + [anywhere] * len(before) + [in_vmem] * len(parts),
            out_specs=anywhere,
            scratch_shapes=[pltpu.SemaphoreType.DMA((panel_size, final - first))],
            input_output_aliases={1: 0} if before else {},
            compiler_params=pltpu.CompilerParams(vmem_limit_bytes=VMEM_GRANT),
        )(info, *before, *parts)
    return out


def solution(mesh):
    seq_size, panel_size = mesh.shape["seq"], mesh.shape["panel"]
    relay = seq_size // CORES - 2 == 2
    if relay:
        body = functools.partial(relayed, seq_size=seq_size, panel_size=panel_size)
    else:
        body = functools.partial(gathered, seq_size=seq_size)
    return jax.shard_map(
        body,
        mesh=mesh,
        in_specs=(
            P(("groups", "seq"), "panel"),
            P(("groups", "seq"), "panel"),
            P(("groups", "seq"), "panel"),
            P("panel", None, None),
            P("panel", None),
        ),
        out_specs=P(("groups", "seq", "panel"), None),
        check_vma=False,
    )
```

```python
import functools

import jax
import jax.numpy as jnp
from jax import lax
from jax.experimental import pallas as pl
from jax.experimental.pallas import tpu as pltpu
from jax.sharding import PartitionSpec as P


HEAD_DIM = 128
BLOCK = 128
LOG2_E = 1.4426950408889634
DEAD = -1e30
CORES = 2
FIRST_SHARE = 7, 12
UNROLL = 5
VMEM_GRANT = 14 << 20
HOMES = 0, 4
STAGES = (
    ("early_0", ((0, 0, (0, 1), False), (0, 1, (0, 1), False)), ()),
    ("early_1", ((0, 0, (2, 3, 4, 5), True), (0, 1, (2, 3), True)), ()),
    (
        "early_2",
        ((1, 0, (0, 1, 2, 3, 4, 5), False),),
        (("chunk", 1, 1), ("chunk", 2, 1), ("chunk", 3, 1), ("query", 1, 0)),
    ),
    ("early_3", ((1, 1, (0, 1, 2, 3, 4, 5), False), (0, 1, (4, 5), True)), (("query", 1, 1),)),
    ("late_0", ((1, 0, (6, 7), True),), ()),
    ("late_3", ((0, 0, (6, 7), True),), ()),
    ("late_1", ((1, 1, (6, 7), True),), ()),
    ("late_2", ((0, 1, (6, 7), True),), ()),
)


def tables(block_lists, block_counts, owner, seq_size):
    heads, tiles, listed = block_lists.shape
    per_index = tiles // seq_size
    lists = lax.dynamic_slice_in_dim(block_lists, owner * per_index, per_index, 1)
    counts = lax.dynamic_slice_in_dim(block_counts, owner * per_index, per_index, 1)
    slot_live = jnp.arange(listed, dtype=jnp.int32) < counts[:, :, None]
    ids = jnp.arange(tiles, dtype=jnp.int32)
    hits = (lists[:, :, :, None] == ids) & slot_live[:, :, :, None]
    keep = jnp.any(hits, axis=2).astype(jnp.int32).reshape(heads, per_index, seq_size, per_index)
    low, high = keep[..., 0], keep[..., 1]
    taken = jnp.max(high, axis=1)
    live = jnp.where(taken[:, None, :] == 1, high, low)
    other = jnp.where(taken[:, None, :] == 1, low, high)
    bits = jnp.array([2 << tile for tile in range(per_index)], jnp.int32)[None, :, None]
    code = taken + jnp.sum(live * bits, axis=1)
    code_other = (1 - taken) + jnp.sum(other * bits, axis=1)
    mine = jnp.arange(seq_size) == owner
    extra = jnp.sum(jnp.where(mine, code_other, 0), axis=1, keepdims=True)
    return jnp.concatenate([code, extra], axis=1)


def attend(query, codes, key_block, value_block):
    rows = query.shape[0]
    factor = HEAD_DIM ** (-0.5) * LOG2_E
    masked = []
    for j, code in enumerate(codes):
        scores = lax.dot_general(
            query, key_block(j, code & 1), (((1,), (1,)), ((), ())), preferred_element_type=jnp.float32
        )
        parts = []
        for tile in range(rows // BLOCK):
            bias = jnp.where((code >> (tile + 1)) & 1 == 1, 0.0, DEAD).astype(jnp.float32)
            parts.append(scores[tile * BLOCK : (tile + 1) * BLOCK] * factor + bias)
        masked.append(jnp.concatenate(parts, axis=0))
    top = jnp.max(functools.reduce(jnp.maximum, masked), axis=1, keepdims=True)
    total, mixed = None, None
    for j, code in enumerate(codes):
        weights = jnp.exp2(masked[j] - top)
        total = weights if total is None else total + weights
        product = jnp.dot(
            weights.astype(jnp.bfloat16), value_block(j, code & 1), preferred_element_type=jnp.float32
        )
        mixed = product if mixed is None else mixed + product
    return mixed / jnp.sum(total, axis=1, keepdims=True)


def gathered_kernel(seq_size, own_rows, info_ref, code_ref, query_ref, key_ref, value_ref, out_ref):
    head = pl.program_id(0)
    owner = info_ref[0]

    def block(ref):
        def read(j, which):
            index = owner if j == seq_size else j
            return ref[pl.ds(pl.multiple_of(index * own_rows + which * BLOCK, BLOCK), BLOCK), :]

        return read

    codes = [code_ref[head * (seq_size + 1) + j] for j in range(seq_size + 1)]
    out_ref[...] = attend(query_ref[...], codes, block(key_ref), block(value_ref)).astype(out_ref.dtype)


def gathered(queries, key_rows, value_rows, block_lists, block_counts, seq_size):
    rows, width = queries.shape
    heads = width // HEAD_DIM
    position = lax.axis_index("seq")
    keys = lax.all_gather(key_rows, "seq", axis=0, tiled=True)
    values = lax.all_gather(value_rows, "seq", axis=0, tiled=True)
    codes = tables(block_lists, block_counts, position, seq_size).reshape(-1)
    all_rows = keys.shape[0]
    out = pl.pallas_call(
        functools.partial(gathered_kernel, seq_size, rows),
        out_shape=jax.ShapeDtypeStruct((rows, width), queries.dtype),
        grid_spec=pltpu.PrefetchScalarGridSpec(
            num_scalar_prefetch=2,
            grid=(heads,),
            in_specs=[
                pl.BlockSpec((rows, HEAD_DIM), lambda h, *_: (0, h)),
                pl.BlockSpec((all_rows, HEAD_DIM), lambda h, *_: (0, h)),
                pl.BlockSpec((all_rows, HEAD_DIM), lambda h, *_: (0, h)),
            ],
            out_specs=pl.BlockSpec((rows, HEAD_DIM), lambda h, *_: (0, h)),
        ),
        name="attend_gathered",
    )(position.reshape(1), codes, queries, keys, values)
    return lax.all_to_all(out, "panel", split_axis=0, concat_axis=1, tiled=True)


def pieces_of(seq_pairs, panel_size, shift):
    return [
        (source * panel_size + panel, target * panel_size + (panel + shift) % panel_size)
        for source, target in seq_pairs
        for panel in range(panel_size)
    ]


def send(value, pairs, axes="seq"):
    return lax.ppermute(value, axes, pairs)


def pack_kernel(starts, sizes, chunk, *refs):
    sources, out, sems = refs[:-2], refs[-2], refs[-1]
    rows = sources[0].shape[0]
    columns = pl.ds(starts[chunk] * HEAD_DIM, sizes[chunk] * HEAD_DIM)
    copies = [
        pltpu.make_async_copy(ref.at[:, columns], out.at[pl.ds(kind * rows, rows), :], sems.at[kind])
        for kind, ref in enumerate(sources)
    ]
    for copy in copies:
        copy.start()
    for copy in copies:
        copy.wait()


def masked_scores(query, codes, key_block):
    factor = HEAD_DIM ** (-0.5) * LOG2_E
    masked = []
    for j, code in codes:
        scores = lax.dot_general(
            key_block(j, code & 1), query, (((1,), (1,)), ((), ())), preferred_element_type=jnp.float32
        )
        tiles = query.shape[0] // BLOCK
        bias = [
            jnp.full((1, BLOCK), jnp.where((code >> (tile + 1)) & 1 == 1, 0.0, DEAD), jnp.float32)
            for tile in range(tiles)
        ]
        masked.append(scores * factor + jnp.concatenate(bias, axis=1))
    return masked


def weigh(masked, top, codes, value_block):
    total, mixed = None, None
    for scores, (j, code) in zip(masked, codes):
        weights = jnp.exp2(scores - top)
        total = weights if total is None else total + weights
        product = lax.dot_general(
            value_block(j, code & 1),
            weights.astype(jnp.bfloat16),
            (((0,), (0,)), ((), ())),
            preferred_element_type=jnp.float32,
        )
        mixed = product if mixed is None else mixed + product
    return jnp.sum(total, axis=0, keepdims=True), mixed


def highest(masked):
    return jnp.max(functools.reduce(jnp.maximum, masked), axis=0, keepdims=True)


def each_unit(count, unit):
    groups = -(-count // UNROLL)
    size = -(-count // groups)
    whole = count // size

    @pl.loop(0, whole)
    def _(group):
        for i in range(size):
            unit(group * size, i)

    for i in range(count - whole * size):
        unit(whole * size, i)


def columns_of(head):
    return pl.ds(pl.multiple_of(head * HEAD_DIM, HEAD_DIM), HEAD_DIM)


def block_reader(pick):
    def block(slot, which):
        ref, first, columns = pick(slot)
        return ref[pl.ds(pl.multiple_of(first + which * BLOCK, BLOCK), BLOCK), columns]

    return block


def stage_kernel(seq_size, panel_size, heads, starts, sizes, jobs, keeps, inputs, final, *refs):
    info_ref, code_ref = refs[:2]
    have = dict(zip(inputs, refs[2:]))
    results = refs[2 + len(inputs) :]
    panel = info_ref[1]

    def job(n, side, k, slots, carry):
        queries = have["query", side, k]
        rows = queries.shape[0]
        piece = rows // panel_size

        def unit(base, i):
            h = base + i
            local = columns_of(h)
            first = (side * heads + h + starts[k]) * (seq_size + 1)
            codes = [(slot, code_ref[first + slot]) for slot in slots]
            if HOMES[side] in slots:
                codes.append((HOMES[side], code_ref[first + seq_size]))

            def pick(kind, slot):
                if ("chunk", slot, k) in have:
                    return have["chunk", slot, k], kind * rows, local
                return have["whole", slot, kind], 0, columns_of(h + starts[k])

            masked = masked_scores(queries[:, local], codes, block_reader(functools.partial(pick, 0)))
            top = highest(masked)
            if carry:
                stat = have["stat", side, k]
                before = stat[h, pl.ds(0, 1), :]
                top = jnp.maximum(before, top)
                kept = jnp.exp2(before - top)
            total, mixed = weigh(masked, top, codes, block_reader(functools.partial(pick, 1)))
            if carry:
                total = total + kept * stat[h, pl.ds(1, 1), :]
                mixed = mixed + kept * have["sum", side, k][h]
            if final:
                spare = results[-1]
                spare[i] = (mixed * (1.0 / total)).astype(spare.dtype).T
                for shift in range(panel_size):
                    first_row = pl.multiple_of(lax.rem(panel + shift, panel_size) * piece, piece)
                    results[n * panel_size + shift][:, local] = spare[i, pl.ds(first_row, piece), :]
            else:
                sums, stats = results[2 * n : 2 * n + 2]
                sums[h] = mixed
                stats[h, pl.ds(0, 1), :] = top
                stats[h, pl.ds(1, 1), :] = total

        each_unit(sizes[k], unit)

    @pl.when(info_ref[0] == 1)
    def _():
        for n, entry in enumerate(jobs):
            job(n, *entry)
        for n, (kind, which, k) in enumerate(keeps):
            copy = results[2 * len(jobs) + n]
            if kind == "query":
                copy[...] = have[kind, which, k][...]
                continue
            rows = copy.shape[0] // 2
            columns = pl.ds(starts[k] * HEAD_DIM, sizes[k] * HEAD_DIM)
            for half in range(2):
                copy[pl.ds(half * rows, rows), :] = have["whole", which, half][:, columns]


def assemble_kernel(panel_size, starts, sizes, aliased, info_ref, *refs):
    out_ref, sems = refs[-2:]
    refs = refs[1:] if aliased else refs
    count = len(sizes)
    width = out_ref.shape[1] // panel_size
    panel = info_ref[1]
    inner = info_ref[0] == 1
    copies = []
    for shift in range(panel_size):
        source = lax.rem(panel + panel_size - shift, panel_size)
        for chunk, (start, size) in enumerate(zip(starts, sizes)):
            columns = pl.ds(pl.multiple_of(source * width + start * HEAD_DIM, HEAD_DIM), size * HEAD_DIM)
            own, guest = (
                pltpu.make_async_copy(
                    refs[(side * count + chunk) * panel_size + shift],
                    out_ref.at[:, columns],
                    sems.at[shift, chunk],
                )
                for side in range(2)
            )
            pl.when(inner)(own.start)
            pl.when(jnp.logical_not(inner))(guest.start)
            copies.append(own)
    for copy in copies:
        copy.wait()


def relayed(queries, key_rows, value_rows, block_lists, block_counts, seq_size, panel_size):
    rows, width = queries.shape
    heads = width // HEAD_DIM
    chips = seq_size // CORES
    position = lax.axis_index("seq")
    panel = lax.axis_index("panel")
    chip, core = position // CORES, position % CORES
    last = chips - 1
    cores = range(CORES)
    inward = [(source * CORES + c, target * CORES + c) for source, target in ((0, 1), (last, last - 1)) for c in cores]
    across = [(source * CORES + c, target * CORES + c) for source, target in ((1, 2), (2, 1)) for c in cores]
    partner = [(z * CORES + c, z * CORES + CORES - 1 - c) for z in (1, 2) for c in cores]
    inner = [(z * CORES + c, z * CORES + c) for z in (1, 2) for c in cores]
    outward = [(target, source) for source, target in inward]
    in_vmem, in_smem, anywhere = (pl.BlockSpec(memory_space=s) for s in (pltpu.VMEM, pltpu.SMEM, pl.ANY))

    front = max(1, heads * FIRST_SHARE[0] // FIRST_SHARE[1])
    sizes = [front, heads - front]
    starts = [0, front]
    chunks = len(sizes)

    middle = [send(x, across) for x in (key_rows, value_rows)]

    def pack(chunk, *sources):
        return pl.pallas_call(
            functools.partial(pack_kernel, starts, sizes, chunk),
            out_shape=jax.ShapeDtypeStruct((len(sources) * rows, sizes[chunk] * HEAD_DIM), sources[0].dtype),
            in_specs=[anywhere] * len(sources),
            out_specs=in_vmem,
            scratch_shapes=[pltpu.SemaphoreType.DMA((len(sources),))],
            compiler_params=pltpu.CompilerParams(vmem_limit_bytes=VMEM_GRANT),
        )(*sources)

    packed = [pack(k, key_rows, value_rows) for k in range(chunks)]
    own_queries = [pack(k, queries) for k in range(chunks)]
    beside = [send(x, partner) for x in (key_rows, value_rows)]
    ends = [send(x, inward) for x in packed]
    guest_queries = [send(x, inward) for x in own_queries]
    middle_beside = [send(x, partner) for x in middle]

    is_inner = (chip >= 1) & (chip < last)
    end = jnp.where(chip * 2 < chips, 0, last)
    guest = end * CORES + core
    order = jnp.stack(
        [
            z * CORES + c
            for z in (chip, last - chip, end, last - end)
            for c in (core, CORES - 1 - core)
        ]
    )
    pick = (order[:, None] == jnp.arange(seq_size)).astype(jnp.int32)

    def arranged(owner):
        codes = tables(block_lists, block_counts, owner, seq_size)
        return jnp.concatenate([jnp.sum(codes[:, None, :seq_size] * pick, axis=2), codes[:, seq_size:]], axis=1)

    codes = jnp.stack([arranged(position), arranged(guest)]).reshape(-1)
    info = jnp.stack([is_inner.astype(jnp.int32), panel])

    ends_beside = [send(x, partner) for x in ends]
    far = [send(x, across) for x in ends]
    far_beside = [send(x, partner) for x in far]
    arrays = {}
    for slot, pair in ((1, beside), (2, middle), (3, middle_beside)):
        for kind in range(2):
            arrays["whole", slot, kind] = pair[kind]
    for k in range(chunks):
        arrays["query", 0, k], arrays["query", 1, k] = own_queries[k], guest_queries[k]
        for slot, parts in ((0, packed), (4, ends), (5, ends_beside), (6, far), (7, far_beside)):
            arrays["chunk", slot, k] = parts[k]

    pieces = {}
    both = ("seq", "panel")
    for name, jobs, keeps in STAGES:
        final = name.startswith("late")
        inputs = []
        for side, k, slots, carry in jobs:
            inputs.append(("query", side, k))
            for slot in slots:
                one = ("chunk", slot, k)
                inputs += [one] if one in arrays else [("whole", slot, kind) for kind in range(2)]
            if carry:
                inputs += [("sum", side, k), ("stat", side, k)]
        inputs = list(dict.fromkeys(inputs))
        if final:
            shapes = [
                jax.ShapeDtypeStruct((rows // panel_size, sizes[k] * HEAD_DIM), queries.dtype)
                for _, k, _, _ in jobs
                for _ in range(panel_size)
            ]
        else:
            shapes = [
                jax.ShapeDtypeStruct((sizes[k], height, rows), jnp.float32)
                for _, k, _, _ in jobs
                for height in (HEAD_DIM, 8)
            ]
            shapes += [
                jax.ShapeDtypeStruct(((1 if kind == "query" else 2) * rows, sizes[k] * HEAD_DIM), queries.dtype)
                for kind, _, k in keeps
            ]
        blocks = sum(sizes[k] * (len(slots) + (HOMES[side] in slots)) for side, k, slots, _ in jobs)
        results = pl.pallas_call(
            functools.partial(stage_kernel, seq_size, panel_size, heads, starts, sizes, jobs, keeps, inputs, final),
            out_shape=shapes,
            in_specs=[in_smem] * 2 + [in_vmem] * len(inputs),
            out_specs=[in_vmem] * len(shapes),
            scratch_shapes=[pltpu.VMEM((UNROLL, rows, HEAD_DIM), queries.dtype)] if final else [],
            compiler_params=pltpu.CompilerParams(vmem_limit_bytes=VMEM_GRANT),
            cost_estimate=pl.CostEstimate(
                flops=4 * rows * blocks * BLOCK * HEAD_DIM,
                bytes_accessed=blocks * 4 * BLOCK * HEAD_DIM,
                transcendentals=rows * blocks * BLOCK,
            ),
        )(info, codes, *(arrays[key] for key in inputs))
        if not final:
            for n, (side, k, _, _) in enumerate(jobs):
                arrays["sum", side, k], arrays["stat", side, k] = results[2 * n : 2 * n + 2]
            arrays.update(zip(keeps, results[2 * len(jobs) :]))
            continue
        for n, (side, k, _, _) in enumerate(jobs):
            for shift in range(panel_size):
                piece = results[n * panel_size + shift]
                if side == 1:
                    piece = send(piece, pieces_of(outward, panel_size, shift), both)
                elif shift:
                    piece = send(piece, pieces_of(inner, panel_size, shift), both)
                pieces[side, k, shift] = piece

    out = None
    for first, final in ((0, chunks - 1), (chunks - 1, chunks)):
        parts = [
            pieces[side, k, shift] for side in range(2) for k in range(first, final) for shift in range(panel_size)
        ]
        before = [] if out is None else [out]
        out = pl.pallas_call(
            functools.partial(assemble_kernel, panel_size, starts[first:final], sizes[first:final], len(before)),
            out_shape=jax.ShapeDtypeStruct((rows // panel_size, width * panel_size), queries.dtype),
            in_specs=[in_smem] + [anywhere] * len(before) + [in_vmem] * len(parts),
            out_specs=anywhere,
            scratch_shapes=[pltpu.SemaphoreType.DMA((panel_size, final - first))],
            input_output_aliases={1: 0} if before else {},
            compiler_params=pltpu.CompilerParams(vmem_limit_bytes=VMEM_GRANT),
        )(info, *before, *parts)
    return out


def solution(mesh):
    seq_size, panel_size = mesh.shape["seq"], mesh.shape["panel"]
    relay = seq_size // CORES - 2 == 2
    if relay:
        body = functools.partial(relayed, seq_size=seq_size, panel_size=panel_size)
    else:
        body = functools.partial(gathered, seq_size=seq_size)
    return jax.shard_map(
        body,
        mesh=mesh,
        in_specs=(
            P(("groups", "seq"), "panel"),
            P(("groups", "seq"), "panel"),
            P(("groups", "seq"), "panel"),
            P("panel", None, None),
            P("panel", None),
        ),
        out_specs=P(("groups", "seq", "panel"), None),
        check_vma=False,
    )
```
